256 devices in a mesh: ctx: 128 (over x, y, z), tp: 2 (over core).
Axes of the slice: x: 4, y: 4, z: 8, core: 2. Of those that a mesh axis runs over, the one named last changes fastest.
Arguments:
- queries: bfloat16 [8192, 2560], P('ctx', 'tp'), may hold values from -100 to 100
- projected_keys: bfloat16 [8192, 512], P('ctx', 'tp'), may hold values from -30 to 30
- projected_values: bfloat16 [8192, 512], P('ctx', 'tp'), may hold values from -6 to 6
- hidden: bfloat16 [8192, 5120], P('ctx', 'tp'), may hold values from -6 to 6
- route_ids: int32 [8192, 1], P('ctx'), may hold values from 0 to 15; in each aligned block of 64 rows (0 to 63, 64 to 127, ...) at most 6 rows name the same one
- route_gain: float32 [8192], P('ctx'), may hold values from 0.25 to 1
- w_gate: bfloat16 [128, 5120, 512], P('ctx', None, 'tp'), may hold values from -0.078125 to 0.078125
- w_up: bfloat16 [128, 5120, 512], P('ctx', None, 'tp'), may hold values from -0.078125 to 0.078125
- w_down: bfloat16 [128, 512, 5120], P('ctx', None, 'tp'), may hold values from -0.09375 to 0.09375
Outputs:
- attended: bfloat16 [8192, 2560], P('ctx', 'tp')
- mixed: bfloat16 [8192, 5120], P('ctx', 'tp')
The draws below stay inside these ranges and needn't reach their ends.
Inputs may be any that keep to these rules, and one draw needn't show every extreme that they name: `route_ids`: within the rows of one device (aligned blocks of 64 rows) no expert is named more than 6 times, a bound that some block reaches.
All inputs are finite; a program needn't handle non-finite values.
Results may differ from the reference program's by a relative error of at most 0.0057.
Values may be sent and summed in bfloat16 or wider, within the bound.
A program may use at most 128 MiB of HBM per device.

```python
import math
import jax
import jax.numpy as jnp
import numpy as np
from jax import lax

D = 5120
HEAD_SIZE = 128
QUERY_HEADS = 20
KEY_VALUE_HEADS = 4
EXPERTS = 16
FF = 4096
TOK_DEV = 64
CAP = 6
SEQUENCE_TOKENS = 8192
HOSTS = 8
N_CTX = 128


def drawn_pair(key):
    key_sample = jax.random.normal(jax.random.fold_in(key, 11), (SEQUENCE_TOKENS, KEY_VALUE_HEADS * HEAD_SIZE), jnp.float32)
    query_draw = jax.random.normal(jax.random.fold_in(key, 12), (SEQUENCE_TOKENS, QUERY_HEADS * HEAD_SIZE), jnp.float32)
    return (query_draw, key_sample)


def draw_queries(key, part):
    return drawn_pair(key)[0].astype(jnp.bfloat16)


def draw_projected_keys(key, part):
    return drawn_pair(key)[1].astype(jnp.bfloat16)


def level_of(key, dims, cuts, smallest, high):
    loudness, own = 1.0, jax.random.fold_in(key, 6)
    for dim, parts in cuts:
        draws = jnp.exp(jax.random.uniform(jax.random.fold_in(own, dim), (parts,), jnp.float32, smallest / len(cuts), high / len(cuts)))
        loudness = loudness * jnp.repeat(draws, dims[dim] // parts).reshape([-1 if axis == dim else 1 for axis in range(len(dims))])
    return loudness


def routed_block(stream_key, own, number, rows, count, top, reach, lean):
    sequence = jax.random.permutation(stream_key, count)
    crowded, ordinary = shares(count, rows * top, reach, lean, True), shares(count, rows * top, reach, lean, False)
    places = jnp.arange(count)

    def named(tallies, offset_by):
        used = int((tallies > 0).sum())
        fixed = max(1, used // 4)
        moved = fixed + (places - fixed + offset_by * (used - fixed)) % max(1, count - fixed)
        return jnp.zeros((count,), jnp.int32).at[sequence[jnp.where(places < fixed, places, moved)]].set(jnp.asarray(tallies, jnp.int32))

    tallies = jnp.where(number % 4 == 0, named(crowded, number // 4), named(ordinary, number - number // 4 - 1))
    mixed = jax.random.permutation(jax.random.fold_in(own, 3), count)
    source_of, sink = mixed[0:count // 2 * 2:2], mixed[1:count // 2 * 2:2]
    slack = jnp.minimum(tallies[source_of] - 1, reach - tallies[sink]) // 2
    slack = jnp.where((source_of == sequence[0]) | (sink == sequence[0]) | (tallies[sink] == 0), 0, jnp.maximum(slack, 0))
    moved = jax.random.randint(jax.random.fold_in(own, 4), (count // 2,), 0, 1 << 20) % (slack + 1)
    tallies = tallies.at[source_of].add(-moved).at[sink].add(moved)
    items = jnp.searchsorted(jnp.cumsum(tallies), jnp.arange(rows * top), side="right").astype(jnp.int32)
    grid = items.reshape(top, rows).T
    grid = grid[jax.random.permutation(jax.random.fold_in(own, 1), rows)]
    offset_by = jax.random.randint(jax.random.fold_in(own, 2), (rows, 1), 0, top)
    return jnp.take_along_axis(grid, (jnp.arange(top)[None, :] + offset_by) % top, axis=1)


def shares(count, total, most, skew, full):
    weights = [(1 << 20) // math.isqrt(rank ** skew) + 1 for rank in range(1, count + 1)]
    largest = most if full else min(most, max(-(-total // count), total * weights[0] // sum(weights)))
    least = 1 if total - largest >= count - 1 else 0
    holding, rest = [largest] + [least] * (count - 1), total - largest - least * (count - 1)
    while rest > 0:
        free = [i for i in range(1, count) if holding[i] < largest] or [i for i in range(1, count) if holding[i] < most]
        whole, budget = sum([weights[i] for i in free]), rest
        for i in free:
            addition = min(most - holding[i], max(1, budget * weights[i] // whole), rest)
            holding[i] = holding[i] + addition
            rest = rest - addition
    return np.array(holding)


def gaussian(own_key, shape, deviation, most, shards=(), kind=jnp.bfloat16):
    values = deviation * jax.random.normal(own_key, shape, jnp.float32)
    if shards:
        values = values * level_of(own_key, shape, shards, -0.22, 0.18)
    return jnp.clip(values, -most, most).astype(kind)


def setup_inputs(seed: int = 0) -> dict:
    seeds = jax.random.split(jax.random.key(seed), 10)
    queries = draw_queries(jax.random.fold_in(seeds[9], 71), 0)
    projected_keys = draw_projected_keys(jax.random.fold_in(seeds[9], 71), 0)
    projected_values = gaussian(seeds[2], (SEQUENCE_TOKENS, KEY_VALUE_HEADS * HEAD_SIZE), 1.0, 6.0, ((0, 128), (1, 2)))
    hidden = gaussian(seeds[3], (SEQUENCE_TOKENS, D), 1.0, 6.0, ((0, 128), (1, 2)))
    route_ids_keys = jax.random.split(jax.random.fold_in(seeds[4], 1), SEQUENCE_TOKENS // TOK_DEV)
    route_ids_turns = jax.random.permutation(jax.random.fold_in(seeds[4], 3), SEQUENCE_TOKENS // TOK_DEV)
    route_ids = jax.vmap(lambda own, number: routed_block(jax.random.fold_in(seeds[4], 2), own, number, TOK_DEV, EXPERTS, 1, CAP, 2))(route_ids_keys, route_ids_turns).reshape((SEQUENCE_TOKENS, 1))
    route_gain = jnp.clip(0.25 + 0.75 * jax.random.uniform(seeds[5], (SEQUENCE_TOKENS,), jnp.float32) ** level_of(seeds[5], (SEQUENCE_TOKENS,), ((0, 128),), -0.2, 0.2), 0.25, 1.0)
    w_gate = gaussian(seeds[6], (EXPERTS * HOSTS, D, FF // HOSTS), D ** -0.5, 0.078125, ((0, 128), (2, 2)))
    w_up = gaussian(seeds[7], (EXPERTS * HOSTS, D, FF // HOSTS), D ** -0.5, 0.078125, ((0, 128), (2, 2)))
    w_down = gaussian(seeds[8], (EXPERTS * HOSTS, FF // HOSTS, D), FF ** -0.5, 0.09375, ((0, 128), (2, 2)))
    return dict(queries=queries, projected_keys=projected_keys, projected_values=projected_values, hidden=hidden, route_ids=route_ids, route_gain=route_gain, w_gate=w_gate, w_up=w_up, w_down=w_down)


def attend_all(queries, projected_keys, projected_values):
    head_group = QUERY_HEADS // KEY_VALUE_HEADS
    score_scale = HEAD_SIZE ** -0.5
    query_tensor = queries.reshape(SEQUENCE_TOKENS, KEY_VALUE_HEADS, head_group, HEAD_SIZE).astype(jnp.float32)
    key_tensor = projected_keys.reshape(SEQUENCE_TOKENS, KEY_VALUE_HEADS, HEAD_SIZE).astype(jnp.float32)
    value_tensor = projected_values.reshape(SEQUENCE_TOKENS, KEY_VALUE_HEADS, HEAD_SIZE).astype(jnp.float32)
    key_pos = jnp.arange(SEQUENCE_TOKENS, dtype=jnp.int32)
    block_rows = 512

    def one_block(block_index):
        query_part = lax.dynamic_slice_in_dim(query_tensor, (block_index * block_rows).astype(jnp.int32), block_rows, 0)
        query_pos = (block_index * block_rows + jnp.arange(block_rows, dtype=jnp.int32)).astype(jnp.int32)
        scores = jnp.einsum("qhgd,khd->hgqk", query_part, key_tensor) * score_scale
        allowed = query_pos[:, None] >= key_pos[None, :]
        scores = jnp.where(allowed, scores, -1e30)
        row_max = jnp.max(scores, axis=3, keepdims=True)
        weights = jnp.where(allowed, jnp.exp(scores - row_max), 0.0)
        denom = jnp.sum(weights, axis=3)
        rounded = lax.optimization_barrier(weights.astype(jnp.bfloat16)).astype(jnp.float32)
        result = jnp.einsum("hgqk,khd->qhgd", rounded, value_tensor)
        result = result / jnp.transpose(denom, (2, 0, 1))[..., None]
        return result.reshape(block_rows, QUERY_HEADS * HEAD_SIZE).astype(jnp.bfloat16)

    blocks = lax.map(one_block, jnp.arange(SEQUENCE_TOKENS // block_rows, dtype=jnp.int32))
    return blocks.reshape(SEQUENCE_TOKENS, QUERY_HEADS * HEAD_SIZE)


def experts_all(hidden, route_ids, route_gain, w_gate, w_up, w_down):
    host_count = N_CTX // EXPERTS
    share = FF // host_count
    ids_flat = route_ids[:, 0].astype(jnp.int32)
    chosen = (ids_flat[:, None] == jnp.arange(EXPERTS, dtype=jnp.int32)[None, :]).astype(jnp.int32)
    chosen = chosen.reshape(N_CTX, TOK_DEV, EXPERTS)
    ranking = jnp.sum((jnp.cumsum(chosen, axis=1) - chosen) * chosen, axis=2).reshape(SEQUENCE_TOKENS)
    source = jnp.arange(SEQUENCE_TOKENS, dtype=jnp.int32) // TOK_DEV
    slot_of = ((ids_flat * N_CTX + source) * CAP + ranking).astype(jnp.int32)
    table = jnp.zeros((EXPERTS * N_CTX * CAP, D), jnp.bfloat16).at[slot_of].set(hidden)
    table = table.reshape(EXPERTS, N_CTX * CAP, D)
    gate_grid = w_gate.reshape(EXPERTS, host_count, D, share)
    up_grid = w_up.reshape(EXPERTS, host_count, D, share)
    down_grid = w_down.reshape(EXPERTS, host_count, share, D)

    def one_expert(operands):
        rows_in, gate_w, up_w, down_w = operands
        inputs_f = rows_in.astype(jnp.float32)
        gate_val = jnp.einsum("rd,jdf->rjf", inputs_f, gate_w.astype(jnp.float32))
        up_val = jnp.einsum("rd,jdf->rjf", inputs_f, up_w.astype(jnp.float32))
        inner = lax.optimization_barrier((jax.nn.silu(gate_val) * up_val).astype(jnp.bfloat16)).astype(jnp.float32)
        partial_out = jnp.einsum("rjf,jfd->rjd", inner, down_w.astype(jnp.float32))
        partial_b = lax.optimization_barrier(partial_out.astype(jnp.bfloat16)).astype(jnp.float32)
        return jnp.sum(partial_b, axis=1)

    results = lax.map(one_expert, (table, gate_grid, up_grid, down_grid))
    results = results.reshape(EXPERTS * N_CTX * CAP, D)
    return (results[slot_of] * route_gain[:, None]).astype(jnp.bfloat16)


def reference(queries, projected_keys, projected_values, hidden, route_ids, route_gain, w_gate, w_up, w_down):
    attended = attend_all(queries, projected_keys, projected_values)
    mixed = experts_all(hidden, route_ids, route_gain, w_gate, w_up, w_down)
    return attended, mixed
```

```python
import functools

import jax
import jax.numpy as jnp
from jax import lax
from jax.experimental import pallas as pl
from jax.experimental.pallas import tpu as pltpu
from jax.sharding import PartitionSpec as P

HEAD_SIZE = 128
EXPERTS = 16
CAP = 6
KEY_BLOCK = 512
LOG2E = 1.4426950408889634
NEG = -1e30


def attention_kernel(rows, groups, heads, q_ref, kv_ref, o_ref, kv_buf, m_ref, l_ref, acc_ref, sems):
    me = lax.axis_index("ctx")
    width = groups * HEAD_SIZE
    first = me * rows
    full = first // KEY_BLOCK
    count = full + 1

    def copy(b):
        span = pl.ds(pl.multiple_of(b * KEY_BLOCK, KEY_BLOCK), KEY_BLOCK)
        return pltpu.make_async_copy(kv_ref.at[span], kv_buf.at[span], sems.at[b])

    @pl.loop(0, count)
    def _(b):
        copy(b).start()

    m_ref[...] = jnp.full_like(m_ref, NEG)
    l_ref[...] = jnp.zeros_like(l_ref)
    acc_ref[...] = jnp.zeros_like(acc_ref)
    scale = HEAD_SIZE ** (-0.5) * LOG2E

    def block(b, masked):
        copy(b).wait()
        span = pl.ds(pl.multiple_of(b * KEY_BLOCK, KEY_BLOCK), KEY_BLOCK)
        for g in range(groups):
            k = kv_buf[span, g * HEAD_SIZE : (g + 1) * HEAD_SIZE]
            v = kv_buf[span, width + g * HEAD_SIZE : width + (g + 1) * HEAD_SIZE]
            for h in range(heads):
                i = g * heads + h
                q = q_ref[:, i * HEAD_SIZE : (i + 1) * HEAD_SIZE]
                s = lax.dot_general(q, k, (((1,), (1,)), ((), ())), preferred_element_type=jnp.float32) * scale
                if masked:
                    row = first + lax.broadcasted_iota(jnp.int32, s.shape, 0)
                    col = b * KEY_BLOCK + lax.broadcasted_iota(jnp.int32, s.shape, 1)
                    s = jnp.where(row >= col, s, NEG)
                m_old = m_ref[i]
                m_new = jnp.maximum(m_old, jnp.max(s, axis=1, keepdims=True))
                p = jnp.exp2(s - m_new[:, :1])
                f = jnp.exp2(m_old - m_new)
                l_ref[i] = l_ref[i] * f + jnp.sum(p, axis=1, keepdims=True)
                acc_ref[i] = acc_ref[i] * f + jnp.dot(p.astype(jnp.bfloat16), v, preferred_element_type=jnp.float32)
                m_ref[i] = m_new

    @pl.loop(0, full)
    def _(b):
        block(b, False)

    block(full, True)
    for i in range(groups * heads):
        o_ref[:, i * HEAD_SIZE : (i + 1) * HEAD_SIZE] = (acc_ref[i] / l_ref[i]).astype(jnp.bfloat16)


def attention(queries, kv_whole):
    rows, width_q = queries.shape
    total, width_kv = kv_whole.shape
    groups = width_kv // 2 // HEAD_SIZE
    q_heads = width_q // HEAD_SIZE
    return pl.pallas_call(
        functools.partial(attention_kernel, rows, groups, q_heads // groups),
        name="attention",
        out_shape=jax.ShapeDtypeStruct((rows, width_q), jnp.bfloat16),
        in_specs=[pl.BlockSpec(memory_space=pltpu.VMEM), pl.BlockSpec(memory_space=pl.ANY)],
        out_specs=pl.BlockSpec(memory_space=pltpu.VMEM),
        scratch_shapes=[
            pltpu.VMEM((total, width_kv), jnp.bfloat16),
            pltpu.VMEM((q_heads, rows, HEAD_SIZE), jnp.float32),
            pltpu.VMEM((q_heads, rows, HEAD_SIZE), jnp.float32),
            pltpu.VMEM((q_heads, rows, HEAD_SIZE), jnp.float32),
            pltpu.SemaphoreType.DMA((total // KEY_BLOCK,)),
        ],
        compiler_params=pltpu.CompilerParams(vmem_limit_bytes=40 * 1024 * 1024),
        cost_estimate=pl.CostEstimate(flops=2 * 2 * rows * width_q * total, bytes_accessed=2 * total * width_kv, transcendentals=0),
    )(queries, kv_whole)


def body(queries, projected_keys, projected_values, hidden, route_ids, route_gain, w_gate, w_up, w_down):
    ctx_count = lax.axis_size("ctx")
    hosts = ctx_count // EXPERTS
    half = hidden.shape[1]
    plane = [[e * hosts + z for e in range(EXPERTS)] for z in range(hosts)]
    column = [[e * hosts + z for z in range(hosts)] for e in range(EXPERTS)]

    kv_whole = lax.all_gather(jnp.concatenate([projected_keys, projected_values], axis=1), "ctx", axis=0, tiled=True)

    ids = route_ids[:, 0]
    chosen = (ids[:, None] == jnp.arange(EXPERTS, dtype=jnp.int32)[None, :]).astype(jnp.int32)
    ranking = jnp.sum((jnp.cumsum(chosen, axis=0) - chosen) * chosen, axis=1)
    slot_of = ids * CAP + ranking
    selector = (jnp.arange(EXPERTS * CAP, dtype=jnp.int32)[:, None] == slot_of[None, :]).astype(jnp.bfloat16)
    packed = jnp.dot(selector, hidden, preferred_element_type=jnp.float32).astype(jnp.bfloat16)
    packed = packed.reshape(EXPERTS, CAP, half)
    arrived = lax.all_to_all(packed, "ctx", 0, 0, axis_index_groups=plane, tiled=True)
    arrived = arrived.reshape(EXPERTS * CAP, half)
    rows = lax.all_gather(arrived, "ctx", axis=0, axis_index_groups=column, tiled=True)
    rows = lax.all_gather(rows, "tp", axis=1, tiled=True)
    gate = jnp.dot(rows, w_gate[0], preferred_element_type=jnp.float32)
    up = jnp.dot(rows, w_up[0], preferred_element_type=jnp.float32)
    inner = (jax.nn.silu(gate) * up).astype(jnp.bfloat16)
    inner = lax.all_gather(inner, "tp", axis=1, tiled=True)
    part = jnp.dot(inner, w_down[0], preferred_element_type=jnp.float32).astype(jnp.bfloat16)
    total = lax.psum_scatter(part, "ctx", scatter_dimension=0, axis_index_groups=column, tiled=True)
    back = lax.all_to_all(total.reshape(EXPERTS, CAP, half), "ctx", 0, 0, axis_index_groups=plane, tiled=True)
    back = back.reshape(EXPERTS * CAP, half)
    own = lax.dot_general(selector, back, (((0,), (0,)), ((), ())), preferred_element_type=jnp.float32)
    mixed = (own * route_gain[:, None]).astype(jnp.bfloat16)
    attended = attention(queries, kv_whole)
    return attended, mixed


def solution(mesh):
    in_specs = (
        P("ctx", "tp"),
        P("ctx", "tp"),
        P("ctx", "tp"),
        P("ctx", "tp"),
        P("ctx", None),
        P("ctx"),
        P("ctx", None, "tp"),
        P("ctx", None, "tp"),
        P("ctx", None, "tp"),
    )
    out_specs = (P("ctx", "tp"), P("ctx", "tp"))
    return jax.shard_map(body, mesh=mesh, in_specs=in_specs, out_specs=out_specs, check_vma=False)
```

```python
import functools

import jax
import jax.numpy as jnp
from jax import lax
from jax.experimental import pallas as pl
from jax.experimental.pallas import tpu as pltpu
from jax.sharding import PartitionSpec as P

HEAD = 128
EXPERTS = 16
SIDE = 4
HOSTS = 8
CAP = 6
SLOT = 8
LOG2E = 1.4426950408889634
NEG = -1e30
MESH = pl.DeviceIdType.MESH
BF = jnp.bfloat16
F32 = jnp.float32


def iota(shape, dim):
    return lax.broadcasted_iota(jnp.int32, shape, dim)


def dot(a, b):
    return jnp.dot(a, b, preferred_element_type=F32)


def kernel(
    ids_ref, gain_ref, hidden_ref, q_ref, keys_ref, values_ref, wg_ref, wu_ref, wd_ref,
    att_ref, mix_ref,
    packed, a2a_in, rows_all, wgu, wd, inner_all, parts, rs_in, back_out, back_in, sel_ref,
    kv, qs, m_ref, l_ref, acc_ref,
    local_sem, a2a_s, a2a_r, kvz_s, kvz_r, zg_s, zg_r, px_s, px_r, in_s, in_r, kv_s, kv_r, rs_s, rs_r, bk_s, bk_r,
):
    tok, half = hidden_ref.shape
    me = lax.axis_index("ctx")
    core = lax.axis_index("tp")
    z = lax.rem(me, HOSTS)
    p = me // HOSTS
    px, py = p // SIDE, lax.rem(p, SIDE)
    crows = EXPERTS * CAP
    hrows = crows // 2
    block_rows = HOSTS * tok
    kvw = keys_ref.shape[1]
    groups = kvw // HEAD
    heads = q_ref.shape[1] // HEAD // groups

    def zat(d):
        return lax.rem(z + d + HOSTS, HOSTS)

    def dev_z(d):
        return {"ctx": p * HOSTS + zat(d), "tp": core}

    def plane_at(i):
        return lax.rem(p + i, EXPERTS)

    def dev_plane(q):
        return {"ctx": q * HOSTS + z, "tp": core}

    partner = {"ctx": me, "tp": 1 - core}

    def remote(src, dst, s, r, device):
        return pltpu.make_async_remote_copy(
            src_ref=src, dst_ref=dst, send_sem=s, recv_sem=r, device_id=device, device_id_type=MESH
        )

    barrier = pltpu.get_barrier_semaphore()
    greeted = [dev_plane(plane_at(i)) for i in range(1, EXPERTS)] + [dev_z(d) for d in range(1, HOSTS)] + [partner]
    for device in greeted:
        pl.semaphore_signal(barrier, inc=1, device_id=device, device_id_type=MESH)

    own_rows = pl.ds(pl.multiple_of(me * tok, tok), tok)
    local = [
        pltpu.make_async_copy(keys_ref, kv.at[own_rows, pl.ds(0, kvw)], local_sem.at[0]),
        pltpu.make_async_copy(values_ref, kv.at[own_rows, pl.ds(kvw, kvw)], local_sem.at[1]),
        pltpu.make_async_copy(wg_ref.at[0], wgu.at[:, pl.ds(0, wg_ref.shape[2])], local_sem.at[2]),
        pltpu.make_async_copy(wu_ref.at[0], wgu.at[:, pl.ds(wg_ref.shape[2], wg_ref.shape[2])], local_sem.at[3]),
        pltpu.make_async_copy(wd_ref.at[0], wd, local_sem.at[4]),
    ]
    for c in local:
        c.start()

    ids = ids_ref[...]
    chosen = (ids == iota((tok, EXPERTS), 1)).astype(F32)
    before = (iota((tok, tok), 1) < iota((tok, tok), 0)).astype(BF)
    rank = jnp.sum(dot(before, chosen.astype(BF)) * chosen, axis=1, keepdims=True).astype(jnp.int32)
    slot = ids * SLOT + rank
    sel = (slot == iota((tok, EXPERTS * SLOT), 1)).astype(BF)
    sel_ref[...] = sel
    packed[...] = lax.dot_general(
        sel, hidden_ref[...], (((0,), (0,)), ((), ())), preferred_element_type=F32
    ).astype(BF)
    for g in range(groups):
        for h in range(heads):
            i = g * heads + h
            qs[g, h * tok : (h + 1) * tok, :] = q_ref[:, i * HEAD : (i + 1) * HEAD]
    m_ref[...] = jnp.full_like(m_ref, NEG)
    l_ref[...] = jnp.zeros_like(l_ref)
    acc_ref[...] = jnp.zeros_like(acc_ref)

    pl.semaphore_wait(barrier, len(greeted))

    def slot_rows(q):
        return pl.ds(pl.multiple_of(q * SLOT, SLOT), SLOT)

    def a2a(i):
        q = plane_at(i)
        return remote(packed.at[slot_rows(q)], a2a_in.at[slot_rows(p)], a2a_s.at[i], a2a_r.at[i], dev_plane(q))

    for i in range(1, EXPERTS):
        a2a(i).start()
    keep = pltpu.make_async_copy(packed.at[slot_rows(p)], a2a_in.at[slot_rows(p)], local_sem.at[5])
    keep.start()

    local[0].wait()
    local[1].wait()

    def kvz(d):
        return remote(kv.at[own_rows], kv.at[own_rows], kvz_s.at[d], kvz_r.at[d], dev_z(d))

    for d in (1, 7, 2, 6, 3, 5, 4):
        kvz(d).start()

    def shifted(part, d1, d2):
        dx, dy = (d1, d2) if part == 0 else (d2, d1)
        return lax.rem(px + dx + SIDE, SIDE) * SIDE + lax.rem(py + dy + SIDE, SIDE)

    part_rows = block_rows // 2
    unit = part_rows // 2
    kv_copies = {}

    def kv_copy(name, part, along, s, d1, d2, off, n):
        if name not in kv_copies:
            kv_copies[name] = len(kv_copies)
        k = kv_copies[name]
        rows = pl.ds(pl.multiple_of(shifted(part, d1, d2) * block_rows + part * part_rows + off, unit), n)
        to = shifted(part, s, 0) if along == 1 else shifted(part, 0, s)
        return remote(kv.at[rows], kv.at[rows], kv_s.at[k], kv_r.at[k], dev_plane(to))

    stages = {}
    for part in (0, 1):
        for s in (1, -1):
            fo = 0 if s == 1 else unit
            stages.setdefault("s1", []).append((("s1", part, s), part, 1, s, 0, 0, 0, part_rows))
            stages.setdefault("s2own", []).append((("s2own", part, s), part, 2, s, 0, 0, 0, part_rows))
            stages.setdefault("f1", []).append((("f1", part, s), part, 1, s, -s, 0, fo, unit))
            for d1 in (-1, 1):
                stages.setdefault("s2a", []).append((("s2a", part, s, d1), part, 2, s, d1, 0, 0, part_rows))
            stages.setdefault("f2own", []).append((("f2own", part, s), part, 2, s, 0, -s, fo, unit))
            for off in (0, unit):
                stages.setdefault("s2b", []).append((("s2b", part, s, off), part, 2, s, 2, 0, off, unit))
            for d1 in (-1, 1):
                stages.setdefault("f2a", []).append((("f2a", part, s, d1), part, 2, s, d1, -s, fo, unit))
            stages.setdefault("f2b", []).append((("f2b", part, s), part, 2, s, 2, -s, fo, unit))

    def kv_start(*names):
        for name in names:
            for c in stages[name]:
                kv_copy(*c).start()

    def kv_wait(name):
        for key, part, along, s, d1, d2, off, n in stages[name]:
            e1, e2 = (d1 - s, d2) if along == 1 else (d1, d2 - s)
            k = kv_copies[key]
            rows = pl.ds(pl.multiple_of(shifted(part, e1, e2) * block_rows + part * part_rows + off, unit), n)
            to = shifted(part, s, 0) if along == 1 else shifted(part, 0, s)
            remote(kv.at[rows], kv.at[rows], kv_s.at[k], kv_r.at[k], dev_plane(to)).wait_recv()

    def half_of(direction, a):
        return a % 2 if direction == 0 else 1 - a % 2

    def rows_at(zs, h):
        return rows_all.at[core, zs, pl.ds(h * hrows, hrows)]

    def zg_send(direction, n):
        sign = 1 if direction == 0 else -1
        ref = rows_at(zat(-sign * (n // 2)), half_of(direction, n))
        return remote(ref, ref, zg_s.at[direction, n], zg_r.at[direction, n], dev_z(sign))

    def arrived(direction, a):
        sign = 1 if direction == 0 else -1
        return rows_at(zat(-sign * (a // 2 + 1)), half_of(direction, a))

    def zg_wait(direction, a):
        ref = arrived(direction, a)
        sign = 1 if direction == 0 else -1
        remote(ref, ref, zg_s.at[direction, a], zg_r.at[direction, a], dev_z(sign)).wait_recv()

    def px_copy(direction, a):
        ref = arrived(direction, a)
        n = direction * 7 + a
        return remote(ref, ref, px_s.at[n], px_r.at[n], partner)

    def px_wait(direction, a):
        sign = 1 if direction == 0 else -1
        ref = rows_all.at[1 - core, zat(-sign * (a // 2 + 1)), pl.ds(half_of(direction, a) * hrows, hrows)]
        n = direction * 7 + a
        remote(ref, ref, px_s.at[n], px_r.at[n], partner).wait_recv()

    def arrive(a):
        for direction in (0, 1):
            zg_wait(direction, a)
            if a <= 4:
                zg_send(direction, a + 2).start()
            px_copy(direction, a).start()

    def gate_up(zs):
        both = dot(rows_all[0, zs], wgu[:half, :]) + dot(rows_all[1, zs], wgu[half:, :])
        width = both.shape[1] // 2
        gate, up = both[:, :width], both[:, width:]
        inner_all[core, zs] = (gate / (1.0 + jnp.exp(-gate)) * up).astype(BF)

    def inner_copy(zs):
        ref = inner_all.at[core, zs]
        return remote(ref, ref, in_s.at[zs], in_r.at[zs], partner)

    def inner_wait(zs):
        ref = inner_all.at[1 - core, zs]
        remote(ref, ref, in_s.at[zs], in_r.at[zs], partner).wait_recv()

    width = wg_ref.shape[2]

    def down(zs):
        for c in range(0, half, 512):
            cols = slice(c, c + 512)
            parts[zs, :, cols] = (
                dot(inner_all[0, zs], wd[:width, cols]) + dot(inner_all[1, zs], wd[width:, cols])
            ).astype(BF)

    def pair(f, d):
        @pl.loop(0, 2)
        def _(i):
            f(zat((2 * i - 1) * d))

    for i in range(1, EXPERTS):
        remote(packed.at[slot_rows(p)], a2a_in.at[slot_rows(p)], a2a_s.at[i], a2a_r.at[i], dev_plane(plane_at(i))).wait_recv()
    keep.wait()
    col = iota((crows, EXPERTS * SLOT), 1)
    dense = ((col // SLOT) * CAP + lax.rem(col, SLOT) == iota((crows, EXPERTS * SLOT), 0)) & (lax.rem(col, SLOT) < CAP)
    dense = dense.astype(BF)
    for c in range(0, half, 512):
        rows_all[core, z, :, c : c + 512] = dot(dense, a2a_in[:, c : c + 512]).astype(BF)

    for d in range(1, HOSTS):
        rows = pl.ds(pl.multiple_of((p * HOSTS + zat(-d)) * tok, tok), tok)
        remote(kv.at[rows], kv.at[rows], kvz_s.at[d], kvz_r.at[d], dev_z(d)).wait_recv()
    kv_start("s1", "s2own")
    for n in (0, 1):
        for direction in (0, 1):
            zg_send(direction, n).start()
    own_ref = rows_all.at[core, z]
    own_px = remote(own_ref, own_ref, px_s.at[14], px_r.at[14], partner)
    own_px.start()
    other_ref = rows_all.at[1 - core, z]
    local[2].wait()
    local[3].wait()
    local[4].wait()
    remote(other_ref, other_ref, px_s.at[14], px_r.at[14], partner).wait_recv()
    gate_up(z)

    arrive(0)
    kv_wait("s1")
    kv_start("f1", "s2a")
    inner_copy(z).start()

    arrive(1)
    inner_wait(z)
    down(z)
    kv_wait("s2own")
    kv_start("f2own")

    def ready(d):
        for direction in (0, 1):
            px_wait(direction, 2 * d - 2)
            px_wait(direction, 2 * d - 1)

    arrive(2)
    ready(1)
    pair(gate_up, 1)
    kv_wait("f1")
    kv_start("s2b")
    pair(lambda zs: inner_copy(zs).start(), 1)

    arrive(3)
    pair(inner_wait, 1)
    pair(down, 1)
    kv_wait("s2a")
    kv_start("f2a")

    arrive(4)
    ready(2)
    pair(gate_up, 2)
    pair(lambda zs: inner_copy(zs).start(), 2)

    arrive(5)
    pair(inner_wait, 2)
    pair(down, 2)
    ready(3)
    pair(gate_up, 3)
    kv_wait("s2b")
    kv_start("f2b")
    pair(lambda zs: inner_copy(zs).start(), 3)

    arrive(6)
    pair(inner_wait, 3)
    pair(down, 3)

    def rs_ref(direction, n):
        sign = 1 if direction == 0 else -1
        return parts.at[zat(sign * (4 - (n + 1) // 2)), pl.ds(half_of(direction, n) * hrows, hrows)]

    def rs_send(direction, n):
        sign = 1 if direction == 0 else -1
        return remote(rs_ref(direction, n), rs_in.at[direction, n], rs_s.at[direction, n], rs_r.at[direction, n], dev_z(sign))

    def rs_step(n):
        for direction in (0, 1):
            rs_send(direction, n - 2).wait_recv()
            ref = rs_ref(direction, n)
            ref[...] = (ref[...].astype(F32) + rs_in[direction, n - 2].astype(F32)).astype(BF)

    def rs_go(n):
        for direction in (0, 1):
            rs_send(direction, n).start()

    px_wait(0, 6)
    px_wait(1, 6)
    rs_go(1)
    far = zat(4)
    gate_up(far)
    kv_wait("f2own")
    inner_copy(far).start()
    inner_wait(far)
    down(far)

    scale = HEAD ** (-0.5) * LOG2E

    def attend(b, masked):
        rows = pl.ds(pl.multiple_of(b * block_rows, block_rows), block_rows)
        for g in range(groups):
            k = kv[rows, g * HEAD : (g + 1) * HEAD]
            v = kv[rows, kvw + g * HEAD : kvw + (g + 1) * HEAD]
            s = lax.dot_general(qs[g], k, (((1,), (1,)), ((), ())), preferred_element_type=F32) * scale
            if masked:
                row = z * tok + lax.rem(iota(s.shape, 0), tok)
                s = jnp.where(iota(s.shape, 1) <= row, s, NEG)
            tiles = [s[:, j : j + HEAD] for j in range(0, block_rows, HEAD)]
            top = functools.reduce(jnp.maximum, tiles)
            m_old = m_ref[g]
            m_new = jnp.maximum(m_old, jnp.max(top, axis=1, keepdims=True))
            w = [jnp.exp2(t - m_new) for t in tiles]
            f = jnp.exp2(m_old - m_new)
            m_ref[g] = m_new
            l_ref[g] = l_ref[g] * f + functools.reduce(jnp.add, w)
            wb = jnp.concatenate([t.astype(BF) for t in w], axis=1)
            acc_ref[g] = acc_ref[g] * f + dot(wb, v)

    def attend_share(n, of):
        @pl.loop(p * n // of, p * (n + 1) // of)
        def _(b):
            attend(b, False)

    kv_wait("f2a")
    rs_go(0)
    rs_step(3)
    attend(p, True)
    rs_go(3)
    rs_step(2)
    kv_wait("f2b")
    rs_go(2)
    attend_share(0, 4)
    rs_step(5)
    rs_go(5)
    attend_share(1, 4)
    rs_step(4)
    rs_go(4)
    attend_share(2, 4)
    rs_step(6)
    rs_go(6)
    attend_share(3, 4)
    for g in range(groups):
        out = acc_ref[g] / jnp.sum(l_ref[g], axis=1, keepdims=True)
        for h in range(heads):
            i = g * heads + h
            att_ref[:, i * HEAD : (i + 1) * HEAD] = out[h * tok : (h + 1) * tok].astype(BF)

    for n in (5, 6):
        for direction in (0, 1):
            rs_send(direction, n).wait_recv()
    srow = iota((EXPERTS * SLOT // 2, hrows), 0)
    spread = ((srow // SLOT) * CAP + lax.rem(srow, SLOT) == iota((EXPERTS * SLOT // 2, hrows), 1)) & (
        lax.rem(srow, SLOT) < CAP
    )
    spread = spread.astype(BF)
    for h in (0, 1):
        right, left = (6, 5) if h == 0 else (5, 6)
        total = (
            parts[z, h * hrows : (h + 1) * hrows, :].astype(F32)
            + rs_in[0, right].astype(F32)
            + rs_in[1, left].astype(F32)
        ).astype(BF)
        n = EXPERTS * SLOT // 2
        back_out[h * n : (h + 1) * n, :] = dot(spread, total).astype(BF)

    def back(i):
        q = plane_at(i)
        return remote(back_out.at[slot_rows(q)], back_in.at[slot_rows(p)], bk_s.at[i], bk_r.at[i], dev_plane(q))

    for i in range(1, EXPERTS):
        back(i).start()
    stay = pltpu.make_async_copy(back_out.at[slot_rows(p)], back_in.at[slot_rows(p)], local_sem.at[6])
    stay.start()

    for i in range(1, EXPERTS):
        a2a(i).wait_send()
    for d in range(1, HOSTS):
        kvz(d).wait_send()
    for n in range(7):
        for direction in (0, 1):
            zg_send(direction, n).wait_send()
            px_copy(direction, n).wait_send()
            rs_send(direction, n).wait_send()
    own_px.wait_send()
    for zs in range(HOSTS):
        inner_copy(zs).wait_send()
    for name in stages:
        for c in stages[name]:
            kv_copy(*c).wait_send()

    for i in range(1, EXPERTS):
        back(i).wait_recv()
    stay.wait()
    for c in range(0, half, 512):
        own = dot(sel_ref[...], back_in[:, c : c + 512])
        mix_ref[:, c : c + 512] = (own * gain_ref[...]).astype(BF)
    for i in range(1, EXPERTS):
        back(i).wait_send()


def body(queries, keys, values, hidden, route_ids, route_gain, w_gate, w_up, w_down):
    tok, half = hidden.shape
    width_q, kvw = queries.shape[1], keys.shape[1]
    ff = w_gate.shape[2]
    total = tok * HOSTS * EXPERTS
    crows = EXPERTS * CAP
    groups = kvw // HEAD
    qrows = width_q // kvw * tok
    vm = pl.BlockSpec(memory_space=pltpu.VMEM)
    hbm = pl.BlockSpec(memory_space=pl.ANY)
    dma = pltpu.SemaphoreType.DMA
    return pl.pallas_call(
        kernel,
        name="layer",
        out_shape=(
            jax.ShapeDtypeStruct((tok, width_q), BF),
            jax.ShapeDtypeStruct((tok, half), BF),
        ),
        in_specs=[vm, vm, vm, vm, hbm, hbm, hbm, hbm, hbm],
        out_specs=(vm, vm),
        scratch_shapes=[
            pltpu.VMEM((EXPERTS * SLOT, half), BF),
            pltpu.VMEM((EXPERTS * SLOT, half), BF),
            pltpu.VMEM((2, HOSTS, crows, half), BF),
            pltpu.VMEM((2 * half, 2 * ff), BF),
            pltpu.VMEM((2 * ff, half), BF),
            pltpu.VMEM((2, HOSTS, crows, ff), BF),
            pltpu.VMEM((HOSTS, crows, half), BF),
            pltpu.VMEM((2, 7, crows // 2, half), BF),
            pltpu.VMEM((EXPERTS * SLOT, half), BF),
            pltpu.VMEM((EXPERTS * SLOT, half), BF),
            pltpu.VMEM((tok, EXPERTS * SLOT), BF),
            pltpu.VMEM((total, 2 * kvw), BF),
            pltpu.VMEM((groups, qrows, HEAD), BF),
            pltpu.VMEM((groups, qrows, HEAD), F32),
            pltpu.VMEM((groups, qrows, HEAD), F32),
            pltpu.VMEM((groups, qrows, HEAD), F32),
            dma((7,)),
            dma((EXPERTS,)), dma((EXPERTS,)),
            dma((HOSTS,)), dma((HOSTS,)),
            dma((2, 7)), dma((2, 7)),
            dma((15,)), dma((15,)),
            dma((HOSTS,)), dma((HOSTS,)),
            dma((44,)), dma((44,)),
            dma((2, 7)), dma((2, 7)),
            dma((EXPERTS,)), dma((EXPERTS,)),
        ],
        compiler_params=pltpu.CompilerParams(
            collective_id=0, has_side_effects=True, vmem_limit_bytes=60 * 1024 * 1024
        ),
    )(route_ids, route_gain[:, None], hidden, queries, keys, values, w_gate, w_up, w_down)


def solution(mesh):
    in_specs = (
        P("ctx", "tp"),
        P("ctx", "tp"),
        P("ctx", "tp"),
        P("ctx", "tp"),
        P("ctx", None),
        P("ctx"),
        P("ctx", None, "tp"),
        P("ctx", None, "tp"),
        P("ctx", None, "tp"),
    )
    out_specs = (P("ctx", "tp"), P("ctx", "tp"))
    return jax.shard_map(body, mesh=mesh, in_specs=in_specs, out_specs=out_specs, check_vma=False)
```

```python
import functools

import jax
import jax.numpy as jnp
from jax import lax
from jax.experimental import pallas as pl
from jax.experimental.pallas import tpu as pltpu
from jax.sharding import PartitionSpec as P

HEAD = 128
EXPERTS = 16
SIDE = 4
HOSTS = 8
CAP = 6
SLOT = 8
LOG2E = 1.4426950408889634
NEG = -1e30
MESH = pl.DeviceIdType.MESH
BF = jnp.bfloat16
F32 = jnp.float32


def iota(shape, dim):
    return lax.broadcasted_iota(jnp.int32, shape, dim)


def dot(a, b):
    return jnp.dot(a, b, preferred_element_type=F32)


def kernel(
    ids_ref, gain_ref, hidden_ref, q_ref, keys_ref, values_ref, wg_ref, wu_ref, wd_ref,
    att_ref, mix_ref,
    hid, qin, packed, a2a_in, rows_all, wgu, wd, inner_all, parts, rs_in, back_out, back_in, sel_ref, gain_col,
    kv, qs, m_ref, l_ref, acc_ref,
    local_sem, a2a_s, a2a_r, kvz_s, kvz_r, zg_s, zg_r, px_s, px_r, in_s, in_r, kv_s, kv_r, rs_s, rs_r, bk_s, bk_r,
):
    tok, half = hidden_ref.shape
    me = lax.axis_index("ctx")
    core = lax.axis_index("tp")
    z = lax.rem(me, HOSTS)
    p = me // HOSTS
    px, py = p // SIDE, lax.rem(p, SIDE)
    crows = EXPERTS * CAP
    hrows = crows // 2
    block_rows = HOSTS * tok
    kvw = keys_ref.shape[1]
    groups = kvw // HEAD
    heads = q_ref.shape[1] // HEAD // groups
    width = wg_ref.shape[2]
    chalf, quarter = half // 2, half // 4

    def zat(d):
        return lax.rem(z + d + HOSTS, HOSTS)

    def dev_z(d):
        return {"ctx": p * HOSTS + zat(d), "tp": core}

    def plane_at(i):
        return lax.rem(p + i, EXPERTS)

    def dev_plane(q):
        return {"ctx": q * HOSTS + z, "tp": core}

    partner = {"ctx": me, "tp": 1 - core}
    signs = (1, -1)

    def remote(src, dst, s, r, device):
        return pltpu.make_async_remote_copy(
            src_ref=src, dst_ref=dst, send_sem=s, recv_sem=r, device_id=device, device_id_type=MESH
        )

    barrier = pltpu.get_barrier_semaphore()
    greeted = [dev_plane(plane_at(i)) for i in range(1, EXPERTS)] + [dev_z(1), dev_z(-1), partner]
    for device in greeted:
        pl.semaphore_signal(barrier, inc=1, device_id=device, device_id_type=MESH)

    own_rows = pl.ds(pl.multiple_of(me * tok, tok), tok)
    local = [
        pltpu.make_async_copy(hidden_ref, hid, local_sem.at[0]),
        pltpu.make_async_copy(keys_ref, kv.at[own_rows, pl.ds(0, kvw)], local_sem.at[1]),
        pltpu.make_async_copy(values_ref, kv.at[own_rows, pl.ds(kvw, kvw)], local_sem.at[2]),
        pltpu.make_async_copy(q_ref, qin, local_sem.at[3]),
        pltpu.make_async_copy(wg_ref.at[0], wgu.at[:, pl.ds(0, width)], local_sem.at[4]),
        pltpu.make_async_copy(wu_ref.at[0], wgu.at[:, pl.ds(width, width)], local_sem.at[5]),
        pltpu.make_async_copy(wd_ref.at[0], wd, local_sem.at[6]),
    ]
    for c in local:
        c.start()

    ids = ids_ref[...]
    chosen = (ids == iota((EXPERTS, tok), 0)).astype(F32)
    before = (iota((tok, tok), 0) < iota((tok, tok), 1)).astype(BF)
    rank = jnp.sum(dot(chosen.astype(BF), before) * chosen, axis=0, keepdims=True).astype(jnp.int32)
    sel = (ids * SLOT + rank == iota((EXPERTS * SLOT, tok), 0)).astype(F32)
    sel_ref[...] = sel.T.astype(BF)
    gain_col[...] = jnp.broadcast_to(gain_ref[...], (HEAD, tok)).T
    sel = sel.astype(BF)
    local[0].wait()
    for c in range(0, half, quarter):
        packed[:, c : c + quarter] = dot(sel, hid[:, c : c + quarter]).astype(BF)
    m_ref[...] = jnp.full_like(m_ref, NEG)
    l_ref[...] = jnp.zeros_like(l_ref)
    acc_ref[...] = jnp.zeros_like(acc_ref)
    local[1].wait()
    local[2].wait()

    pl.semaphore_wait(barrier, len(greeted))

    def kvz(direction, n, lag):
        sign = signs[direction]
        start = (p * HOSTS + zat(-sign * (n + lag))) * tok
        if n == 3:
            rows = pl.ds(pl.multiple_of(start + direction * (tok // 2), tok // 2), tok // 2)
        else:
            rows = pl.ds(pl.multiple_of(start, tok), tok)
        return remote(kv.at[rows], kv.at[rows], kvz_s.at[direction, n], kvz_r.at[direction, n], dev_z(sign))

    def kvz_go(n):
        for direction in (0, 1):
            kvz(direction, n, 0).start()

    def kvz_wait(n):
        for direction in (0, 1):
            kvz(direction, n, 1).wait_recv()

    kvz_go(0)

    def slot_rows(q):
        return pl.ds(pl.multiple_of(q * SLOT, SLOT), SLOT)

    def a2a(i, c):
        q = plane_at(i)
        cols = pl.ds(c * quarter, quarter)
        return remote(
            packed.at[slot_rows(q), cols], a2a_in.at[slot_rows(p), cols], a2a_s.at[c, i], a2a_r.at[c, i], dev_plane(q)
        )

    keep = pltpu.make_async_copy(packed.at[slot_rows(p)], a2a_in.at[slot_rows(p)], local_sem.at[7])
    keep.start()
    for c in range(4):
        for i in range(1, EXPERTS):
            a2a(i, c).start()

    def shifted(part, d1, d2):
        dx, dy = (d1, d2) if part == 0 else (d2, d1)
        return lax.rem(px + dx + SIDE, SIDE) * SIDE + lax.rem(py + dy + SIDE, SIDE)

    part_rows = block_rows // 2
    unit = part_rows // 2
    kv_copies = {}

    def kv_copy(name, part, along, s, d1, d2, off, n):
        if name not in kv_copies:
            kv_copies[name] = len(kv_copies)
        k = kv_copies[name]
        rows = pl.ds(pl.multiple_of(shifted(part, d1, d2) * block_rows + part * part_rows + off, unit), n)
        to = shifted(part, s, 0) if along == 1 else shifted(part, 0, s)
        return remote(kv.at[rows], kv.at[rows], kv_s.at[k], kv_r.at[k], dev_plane(to))

    stages = {}
    for part in (0, 1):
        for s in (1, -1):
            fo = 0 if s == 1 else unit
            stages.setdefault("s1", []).append((("s1", part, s), part, 1, s, 0, 0, 0, part_rows))
            stages.setdefault("s2own", []).append((("s2own", part, s), part, 2, s, 0, 0, 0, part_rows))
            stages.setdefault("f1", []).append((("f1", part, s), part, 1, s, -s, 0, fo, unit))
            for d1 in (-1, 1):
                stages.setdefault("s2a", []).append((("s2a", part, s, d1), part, 2, s, d1, 0, 0, part_rows))
            stages.setdefault("f2own", []).append((("f2own", part, s), part, 2, s, 0, -s, fo, unit))
            for off in (0, unit):
                stages.setdefault("s2b", []).append((("s2b", part, s, off), part, 2, s, 2, 0, off, unit))
            for d1 in (-1, 1):
                stages.setdefault("f2a", []).append((("f2a", part, s, d1), part, 2, s, d1, -s, fo, unit))
            stages.setdefault("f2b", []).append((("f2b", part, s), part, 2, s, 2, -s, fo, unit))

    def kv_start(*names):
        for name in names:
            for c in stages[name]:
                kv_copy(*c).start()

    def kv_wait(name):
        for key, part, along, s, d1, d2, off, n in stages[name]:
            e1, e2 = (d1 - s, d2) if along == 1 else (d1, d2 - s)
            k = kv_copies[key]
            rows = pl.ds(pl.multiple_of(shifted(part, e1, e2) * block_rows + part * part_rows + off, unit), n)
            to = shifted(part, s, 0) if along == 1 else shifted(part, 0, s)
            remote(kv.at[rows], kv.at[rows], kv_s.at[k], kv_r.at[k], dev_plane(to)).wait_recv()

    def zg_ref(direction, n, lag):
        sign = signs[direction]
        if n < 4:
            hop, cols, rows = 0, pl.ds(n * quarter, quarter), pl.ds(0, crows)
        else:
            hop, cols = (n - 2) // 2, pl.ds(n % 2 * chalf, chalf)
            rows = pl.ds(direction * hrows, hrows) if n >= 8 else pl.ds(0, crows)
        return rows_all.at[core, zat(-sign * (hop + lag)), rows, cols]

    def zg(direction, n, lag):
        ref = zg_ref(direction, n, lag)
        return remote(ref, ref, zg_s.at[direction, n], zg_r.at[direction, n], dev_z(signs[direction]))

    def px_ref(direction, a, side):
        d, c = a // 2 + 1, a % 2
        rows = pl.ds(direction * hrows, hrows) if d == 4 else pl.ds(0, crows)
        return rows_all.at[side, zat(-signs[direction] * d), rows, pl.ds(c * chalf, chalf)]

    def px_copy(direction, a):
        ref = px_ref(direction, a, core)
        return remote(ref, ref, px_s.at[direction * 8 + a], px_r.at[direction * 8 + a], partner)

    def px_wait(direction, a):
        ref = px_ref(direction, a, 1 - core)
        remote(ref, ref, px_s.at[direction * 8 + a], px_r.at[direction * 8 + a], partner).wait_recv()

    def arrive(a):
        for direction in (0, 1):
            for n in (2 * a, 2 * a + 1) if a < 2 else (a + 2,):
                zg(direction, n, 1).wait_recv()
            if a < 6:
                zg(direction, a + 4, 0).start()
            px_copy(direction, a).start()

    def ready(d):
        for direction in (0, 1):
            px_wait(direction, 2 * d - 2)
            px_wait(direction, 2 * d - 1)

    def gate_up(zs):
        both = dot(rows_all[0, zs], wgu[:half, :]) + dot(rows_all[1, zs], wgu[half:, :])
        gate, up = both[:, :width], both[:, width:]
        inner_all[core, zs] = (gate / (1.0 + jnp.exp(-gate)) * up).astype(BF)

    def inner_copy(zs):
        ref = inner_all.at[core, zs]
        return remote(ref, ref, in_s.at[zs], in_r.at[zs], partner)

    def inner_wait(zs):
        ref = inner_all.at[1 - core, zs]
        remote(ref, ref, in_s.at[zs], in_r.at[zs], partner).wait_recv()

    def down(zs):
        for c in range(0, half, 512):
            cols = slice(c, c + 512)
            parts[zs, :, cols] = (
                dot(inner_all[0, zs], wd[:width, cols]) + dot(inner_all[1, zs], wd[width:, cols])
            ).astype(BF)

    def pair(f, d):
        @pl.loop(0, 2)
        def _(i):
            f(zat((2 * i - 1) * d))

    col = iota((crows, EXPERTS * SLOT), 1)
    dense = ((col // SLOT) * CAP + lax.rem(col, SLOT) == iota((crows, EXPERTS * SLOT), 0)) & (lax.rem(col, SLOT) < CAP)
    dense = dense.astype(BF)
    kvz_wait(0)
    kvz_go(1)
    keep.wait()
    for c in range(4):
        cols = pl.ds(c * quarter, quarter)
        for i in range(1, EXPERTS):
            ref = a2a_in.at[slot_rows(plane_at(EXPERTS - i)), cols]
            remote(ref, ref, a2a_s.at[c, i], a2a_r.at[c, i], dev_plane(plane_at(i))).wait_recv()
        rows_all[core, z, :, c * quarter : (c + 1) * quarter] = dot(
            dense, a2a_in[:, c * quarter : (c + 1) * quarter]
        ).astype(BF)
        if c in (0, 1):
            kvz_wait(c + 1)
            kvz_go(c + 2)
        for direction in (0, 1):
            zg(direction, c, 0).start()
    own_ref = rows_all.at[core, z]
    own_px = remote(own_ref, own_ref, px_s.at[16], px_r.at[16], partner)
    own_px.start()
    kvz_wait(3)
    kv_start("s1", "s2own")
    local[3].wait()
    for g in range(groups):
        for h in range(heads):
            i = g * heads + h
            qs[g, h * tok : (h + 1) * tok, :] = qin[:, i * HEAD : (i + 1) * HEAD]
    other_ref = rows_all.at[1 - core, z]
    local[4].wait()
    local[5].wait()
    local[6].wait()

    arrive(0)
    remote(other_ref, other_ref, px_s.at[16], px_r.at[16], partner).wait_recv()
    gate_up(z)
    kv_wait("s1")
    kv_start("f1", "s2a")
    inner_copy(z).start()

    arrive(1)
    inner_wait(z)
    down(z)
    kv_wait("s2own")
    kv_start("f2own")

    arrive(2)
    ready(1)
    pair(gate_up, 1)
    kv_wait("f1")
    kv_start("s2b")
    pair(lambda zs: inner_copy(zs).start(), 1)

    arrive(3)
    pair(inner_wait, 1)
    pair(down, 1)
    kv_wait("s2a")
    kv_start("f2a")

    arrive(4)
    ready(2)
    pair(gate_up, 2)
    pair(lambda zs: inner_copy(zs).start(), 2)

    arrive(5)
    pair(inner_wait, 2)
    pair(down, 2)
    ready(3)
    pair(gate_up, 3)
    pair(lambda zs: inner_copy(zs).start(), 3)

    def rs_rows(direction, chain):
        return pl.ds((direction ^ chain) * hrows, hrows)

    def rs_part(direction, chain, t, c):
        return parts.at[zat(signs[direction] * t), rs_rows(direction, chain), pl.ds(c * chalf, chalf)]

    def rs_slot(direction, chain, t, c):
        return rs_in.at[direction, chain * 4 + t - 1, :, pl.ds(c * chalf, chalf)]

    def rs(direction, chain, t, c):
        n = (chain * 4 + t - 1) * 2 + c
        return remote(
            rs_part(direction, chain, t, c), rs_slot(direction, chain, t, c),
            rs_s.at[direction, n], rs_r.at[direction, n], dev_z(signs[direction]),
        )

    def rs_add(chain, t, c):
        for direction in (0, 1):
            rs(direction, chain, t + 1, c).wait_recv()
            ref = rs_part(direction, chain, t, c)
            ref[...] = (ref[...].astype(F32) + rs_slot(direction, chain, t + 1, c)[...].astype(F32)).astype(BF)

    def rs_go(chain, t, c):
        for direction in (0, 1):
            rs(direction, chain, t, c).start()

    def rs_step(chain, t, c):
        rs_add(chain, t, c)
        rs_go(chain, t, c)

    scale = HEAD ** (-0.5) * LOG2E

    def attend(b, masked):
        rows = pl.ds(pl.multiple_of(b * block_rows, block_rows), block_rows)
        for g in range(groups):
            k = kv[rows, g * HEAD : (g + 1) * HEAD]
            v = kv[rows, kvw + g * HEAD : kvw + (g + 1) * HEAD]
            s = lax.dot_general(qs[g], k, (((1,), (1,)), ((), ())), preferred_element_type=F32) * scale
            if masked:
                row = z * tok + lax.rem(iota(s.shape, 0), tok)
                s = jnp.where(iota(s.shape, 1) <= row, s, NEG)
            tiles = [s[:, j : j + HEAD] for j in range(0, block_rows, HEAD)]
            top = functools.reduce(jnp.maximum, tiles)
            m_old = m_ref[g]
            m_new = jnp.maximum(m_old, jnp.max(top, axis=1, keepdims=True))
            w = [jnp.exp2(t - m_new) for t in tiles]
            f = jnp.exp2(m_old - m_new)
            m_ref[g] = m_new
            l_ref[g] = l_ref[g] * f + functools.reduce(jnp.add, w)
            wb = jnp.concatenate([t.astype(BF) for t in w], axis=1)
            acc_ref[g] = acc_ref[g] * f + dot(wb, v)

    def attend_share(n, of):
        @pl.loop(p * n // of, p * (n + 1) // of)
        def _(b):
            attend(b, False)

    arrive(6)
    pair(inner_wait, 3)
    pair(down, 3)
    rs_go(1, 3, 0)
    rs_go(1, 3, 1)
    arrive(7)
    far = zat(4)
    ready(4)
    gate_up(far)
    inner_copy(far).start()
    kv_wait("s2b")
    kv_start("f2b")
    inner_wait(far)
    down(far)
    kv_wait("f2own")
    rs_go(0, 4, 0)
    rs_step(1, 2, 0)
    rs_go(0, 4, 1)
    rs_step(1, 2, 1)
    attend(p, True)
    kv_wait("f2a")
    rs_step(0, 3, 0)
    kv_wait("f2b")
    attend_share(0, 4)
    rs_step(0, 3, 1)
    rs_step(1, 1, 0)
    attend_share(1, 4)
    rs_step(0, 2, 0)
    rs_step(0, 2, 1)
    attend_share(2, 4)
    rs_step(0, 1, 0)
    rs_step(1, 1, 1)
    rs_step(0, 1, 1)
    attend_share(3, 4)

    srow = iota((EXPERTS * SLOT // 2, hrows), 0)
    spread = ((srow // SLOT) * CAP + lax.rem(srow, SLOT) == iota((EXPERTS * SLOT // 2, hrows), 1)) & (
        lax.rem(srow, SLOT) < CAP
    )
    spread = spread.astype(BF)

    def back(i, c):
        q = plane_at(i)
        cols = pl.ds(c * chalf, chalf)
        return remote(
            back_out.at[slot_rows(q), cols], back_in.at[slot_rows(p), cols], bk_s.at[c, i], bk_r.at[c, i], dev_plane(q)
        )

    def finish(c):
        for direction in (0, 1):
            rs(direction, 1, 1, c).wait_recv()
            rs(direction, 0, 1, c).wait_recv()
        cols = slice(c * chalf, (c + 1) * chalf)
        for h in (0, 1):
            total = parts[z, h * hrows : (h + 1) * hrows, cols].astype(F32)
            for direction in (0, 1):
                total = total + rs_slot(direction, direction ^ h, 1, c)[...].astype(F32)
            n = EXPERTS * SLOT // 2
            back_out[h * n : (h + 1) * n, cols] = dot(spread, total.astype(BF)).astype(BF)
        stay = pltpu.make_async_copy(
            back_out.at[slot_rows(p), pl.ds(c * chalf, chalf)],
            back_in.at[slot_rows(p), pl.ds(c * chalf, chalf)],
            local_sem.at[8 + c],
        )
        stay.start()
        for i in range(1, EXPERTS):
            back(i, c).start()
        return stay

    def mix(c, stay):
        for i in range(1, EXPERTS):
            ref = back_in.at[slot_rows(plane_at(EXPERTS - i)), pl.ds(c * chalf, chalf)]
            remote(ref, ref, bk_s.at[c, i], bk_r.at[c, i], dev_plane(plane_at(i))).wait_recv()
        stay.wait()
        for b in range(c * chalf, (c + 1) * chalf, quarter):
            own = dot(sel_ref[...], back_in[:, b : b + quarter])
            for t in range(0, quarter, HEAD):
                mix_ref[:, b + t : b + t + HEAD] = (own[:, t : t + HEAD] * gain_col[...]).astype(BF)

    first = finish(0)
    for g in range(groups):
        out = acc_ref[g] / jnp.sum(l_ref[g], axis=1, keepdims=True)
        for h in range(heads):
            i = g * heads + h
            att_ref[:, i * HEAD : (i + 1) * HEAD] = out[h * tok : (h + 1) * tok].astype(BF)
    second = finish(1)

    for c in range(4):
        for i in range(1, EXPERTS):
            a2a(i, c).wait_send()
    for direction in (0, 1):
        for n in range(4):
            kvz(direction, n, 0).wait_send()
        for n in range(10):
            zg(direction, n, 0).wait_send()
        for a in range(8):
            px_copy(direction, a).wait_send()
        for c in (0, 1):
            for t in (4, 3, 2, 1):
                rs(direction, 0, t, c).wait_send()
            for t in (3, 2, 1):
                rs(direction, 1, t, c).wait_send()
    own_px.wait_send()
    for zs in range(HOSTS):
        inner_copy(zs).wait_send()
    for name in stages:
        for c in stages[name]:
            kv_copy(*c).wait_send()

    mix(0, first)
    mix(1, second)
    for c in (0, 1):
        for i in range(1, EXPERTS):
            back(i, c).wait_send()


def body(queries, keys, values, hidden, route_ids, route_gain, w_gate, w_up, w_down):
    tok, half = hidden.shape
    width_q, kvw = queries.shape[1], keys.shape[1]
    ff = w_gate.shape[2]
    total = tok * HOSTS * EXPERTS
    crows = EXPERTS * CAP
    groups = kvw // HEAD
    qrows = width_q // kvw * tok
    vm = pl.BlockSpec(memory_space=pltpu.VMEM)
    hbm = pl.BlockSpec(memory_space=pl.ANY)
    dma = pltpu.SemaphoreType.DMA
    return pl.pallas_call(
        kernel,
        name="layer",
        out_shape=(
            jax.ShapeDtypeStruct((tok, width_q), BF),
            jax.ShapeDtypeStruct((tok, half), BF),
        ),
        in_specs=[vm, vm] + [hbm] * 7,
        out_specs=(vm, vm),
        scratch_shapes=[
            pltpu.VMEM((tok, half), BF),
            pltpu.VMEM((tok, width_q), BF),
            pltpu.VMEM((EXPERTS * SLOT, half), BF),
            pltpu.VMEM((EXPERTS * SLOT, half), BF),
            pltpu.VMEM((2, HOSTS, crows, half), BF),
            pltpu.VMEM((2 * half, 2 * ff), BF),
            pltpu.VMEM((2 * ff, half), BF),
            pltpu.VMEM((2, HOSTS, crows, ff), BF),
            pltpu.VMEM((HOSTS, crows, half), BF),
            pltpu.VMEM((2, 7, crows // 2, half), BF),
            pltpu.VMEM((EXPERTS * SLOT, half), BF),
            pltpu.VMEM((EXPERTS * SLOT, half), BF),
            pltpu.VMEM((tok, EXPERTS * SLOT), BF),
            pltpu.VMEM((tok, HEAD), F32),
            pltpu.VMEM((total, 2 * kvw), BF),
            pltpu.VMEM((groups, qrows, HEAD), BF),
            pltpu.VMEM((groups, qrows, HEAD), F32),
            pltpu.VMEM((groups, qrows, HEAD), F32),
            pltpu.VMEM((groups, qrows, HEAD), F32),
            dma((10,)),
            dma((4, EXPERTS)), dma((4, EXPERTS)),
            dma((2, 4)), dma((2, 4)),
            dma((2, 10)), dma((2, 10)),
            dma((17,)), dma((17,)),
            dma((HOSTS,)), dma((HOSTS,)),
            dma((44,)), dma((44,)),
            dma((2, 14)), dma((2, 14)),
            dma((2, EXPERTS)), dma((2, EXPERTS)),
        ],
        compiler_params=pltpu.CompilerParams(
            collective_id=0, has_side_effects=True, vmem_limit_bytes=60 * 1024 * 1024
        ),
    )(route_ids.reshape(1, tok), route_gain.reshape(1, tok), hidden, queries, keys, values, w_gate, w_up, w_down)


def solution(mesh):
    in_specs = (
        P("ctx", "tp"),
        P("ctx", "tp"),
        P("ctx", "tp"),
        P("ctx", "tp"),
        P("ctx", None),
        P("ctx"),
        P("ctx", None, "tp"),
        P("ctx", None, "tp"),
        P("ctx", None, "tp"),
    )
    out_specs = (P("ctx", "tp"), P("ctx", "tp"))
    return jax.shard_map(body, mesh=mesh, in_specs=in_specs, out_specs=out_specs, check_vma=False)
```

```python
import functools

import jax
import jax.numpy as jnp
from jax import lax
from jax.experimental import pallas as pl
from jax.experimental.pallas import tpu as pltpu
from jax.sharding import PartitionSpec as P

HEAD = 128
EXPERTS = 16
SIDE = 4
HOSTS = 8
CAP = 6
SLOT = 8
LOG2E = 1.4426950408889634
NEG = -1e30
MESH = pl.DeviceIdType.MESH
BF = jnp.bfloat16
F32 = jnp.float32


def iota(shape, dim):
    return lax.broadcasted_iota(jnp.int32, shape, dim)


def dot(a, b):
    return jnp.dot(a, b, preferred_element_type=F32)


def kernel(
    ids_ref, gain_ref, hidden_ref, q_ref, keys_ref, values_ref, wg_ref, wu_ref, wd_ref,
    att_hbm, mix_hbm,
    att_ref, mix_ref, hid, qin, packed, a2a_in, rows_all, wgu, wd, inner_all, parts, rs_in, back_out, back_in, sel_ref, gain_col,
    kv, qs, m_ref, l_ref, acc_ref,
    local_sem, a2a_s, a2a_r, kvz_s, kvz_r, zg_s, zg_r, px_s, px_r, in_s, in_r, kv_s, kv_r, rs_s, rs_r, bk_s, bk_r,
):
    tok, half = hidden_ref.shape
    me = lax.axis_index("ctx")
    core = lax.axis_index("tp")
    z = lax.rem(me, HOSTS)
    p = me // HOSTS
    px, py = p // SIDE, lax.rem(p, SIDE)
    crows = EXPERTS * CAP
    hrows = crows // 2
    block_rows = HOSTS * tok
    kvw = keys_ref.shape[1]
    groups = kvw // HEAD
    heads = q_ref.shape[1] // HEAD // groups
    width = wg_ref.shape[2]
    chalf, quarter = half // 2, half // 4

    def zat(d):
        return lax.rem(z + d + HOSTS, HOSTS)

    def dev_z(d):
        return {"ctx": p * HOSTS + zat(d), "tp": core}

    def plane_at(i):
        return lax.rem(p + i, EXPERTS)

    def dev_plane(q):
        return {"ctx": q * HOSTS + z, "tp": core}

    partner = {"ctx": me, "tp": 1 - core}
    signs = (1, -1)

    def remote(src, dst, s, r, device):
        return pltpu.make_async_remote_copy(
            src_ref=src, dst_ref=dst, send_sem=s, recv_sem=r, device_id=device, device_id_type=MESH
        )

    barrier = pltpu.get_barrier_semaphore()
    greeted = [dev_plane(plane_at(i)) for i in range(1, EXPERTS)] + [dev_z(1), dev_z(-1), partner]
    for device in greeted:
        pl.semaphore_signal(barrier, inc=1, device_id=device, device_id_type=MESH)

    own_rows = pl.ds(pl.multiple_of(me * tok, tok), tok)
    local = [
        pltpu.make_async_copy(hidden_ref, hid, local_sem.at[0]),
        pltpu.make_async_copy(keys_ref, kv.at[own_rows, pl.ds(0, kvw)], local_sem.at[1]),
        pltpu.make_async_copy(values_ref, kv.at[own_rows, pl.ds(kvw, kvw)], local_sem.at[2]),
        pltpu.make_async_copy(q_ref, qin, local_sem.at[3]),
        pltpu.make_async_copy(wg_ref.at[0], wgu.at[:, pl.ds(0, width)], local_sem.at[4]),
        pltpu.make_async_copy(wu_ref.at[0], wgu.at[:, pl.ds(width, width)], local_sem.at[5]),
        pltpu.make_async_copy(wd_ref.at[0], wd, local_sem.at[6]),
    ]
    for c in local:
        c.start()

    ids = ids_ref[...]
    chosen = (ids == iota((EXPERTS, tok), 0)).astype(F32)
    before = (iota((tok, tok), 0) < iota((tok, tok), 1)).astype(BF)
    rank = jnp.sum(dot(chosen.astype(BF), before) * chosen, axis=0, keepdims=True).astype(jnp.int32)
    sel = (ids * SLOT + rank == iota((EXPERTS * SLOT, tok), 0)).astype(F32)
    sel_ref[...] = sel.T.astype(BF)
    gain_col[...] = jnp.broadcast_to(gain_ref[...], (HEAD, tok)).T
    sel = sel.astype(BF)
    local[0].wait()
    for c in range(0, half, quarter):
        packed[:, :, c : c + quarter] = dot(sel, hid[:, c : c + quarter]).reshape(EXPERTS, SLOT, quarter).astype(BF)
    m_ref[...] = jnp.full_like(m_ref, NEG)
    l_ref[...] = jnp.zeros_like(l_ref)
    acc_ref[...] = jnp.zeros_like(acc_ref)
    unread = jnp.zeros((EXPERTS, SLOT - CAP, half), BF)
    a2a_in[:, CAP:, :] = unread
    back_in[:, CAP:, :] = unread
    local[1].wait()
    local[2].wait()

    pl.semaphore_wait(barrier, len(greeted))

    def kvz(direction, n, lag):
        sign = signs[direction]
        start = (p * HOSTS + zat(-sign * (n + lag))) * tok
        if n == 3:
            rows = pl.ds(pl.multiple_of(start + direction * (tok // 2), tok // 2), tok // 2)
        else:
            rows = pl.ds(pl.multiple_of(start, tok), tok)
        return remote(kv.at[rows], kv.at[rows], kvz_s.at[direction, n], kvz_r.at[direction, n], dev_z(sign))

    def kvz_go(n):
        for direction in (0, 1):
            kvz(direction, n, 0).start()

    def kvz_wait(n):
        for direction in (0, 1):
            kvz(direction, n, 1).wait_recv()

    kvz_go(0)

    def slot_rows(q):
        return q, pl.ds(0, CAP)

    def a2a(i, c):
        q = plane_at(i)
        cols = pl.ds(c * quarter, quarter)
        return remote(
            packed.at[(*slot_rows(q), cols)], a2a_in.at[(*slot_rows(p), cols)], a2a_s.at[c, i], a2a_r.at[c, i], dev_plane(q)
        )

    keep = pltpu.make_async_copy(packed.at[slot_rows(p)], a2a_in.at[slot_rows(p)], local_sem.at[7])
    keep.start()
    for c in range(4):
        for i in range(1, EXPERTS):
            a2a(i, c).start()

    def shifted(part, d1, d2):
        dx, dy = (d1, d2) if part == 0 else (d2, d1)
        return lax.rem(px + dx + SIDE, SIDE) * SIDE + lax.rem(py + dy + SIDE, SIDE)

    part_rows = block_rows // 2
    unit = part_rows // 2
    kv_copies = {}

    def kv_copy(name, part, along, s, d1, d2, off, n):
        if name not in kv_copies:
            kv_copies[name] = len(kv_copies)
        k = kv_copies[name]
        rows = pl.ds(pl.multiple_of(shifted(part, d1, d2) * block_rows + part * part_rows + off, unit), n)
        to = shifted(part, s, 0) if along == 1 else shifted(part, 0, s)
        return remote(kv.at[rows], kv.at[rows], kv_s.at[k], kv_r.at[k], dev_plane(to))

    stages = {}
    for part in (0, 1):
        for s in (1, -1):
            fo = 0 if s == 1 else unit
            stages.setdefault("s1", []).append((("s1", part, s), part, 1, s, 0, 0, 0, part_rows))
            stages.setdefault("s2own", []).append((("s2own", part, s), part, 2, s, 0, 0, 0, part_rows))
            stages.setdefault("f1", []).append((("f1", part, s), part, 1, s, -s, 0, fo, unit))
            for d1 in (-1, 1):
                stages.setdefault("s2a", []).append((("s2a", part, s, d1), part, 2, s, d1, 0, 0, part_rows))
            stages.setdefault("f2own", []).append((("f2own", part, s), part, 2, s, 0, -s, fo, unit))
            for off in (0, unit):
                stages.setdefault("s2b", []).append((("s2b", part, s, off), part, 2, s, 2, 0, off, unit))
            for d1 in (-1, 1):
                stages.setdefault("f2a", []).append((("f2a", part, s, d1), part, 2, s, d1, -s, fo, unit))
            stages.setdefault("f2b", []).append((("f2b", part, s), part, 2, s, 2, -s, fo, unit))

    def kv_start(*names):
        for name in names:
            for c in stages[name]:
                kv_copy(*c).start()

    def kv_wait(name):
        for key, part, along, s, d1, d2, off, n in stages[name]:
            e1, e2 = (d1 - s, d2) if along == 1 else (d1, d2 - s)
            k = kv_copies[key]
            rows = pl.ds(pl.multiple_of(shifted(part, e1, e2) * block_rows + part * part_rows + off, unit), n)
            to = shifted(part, s, 0) if along == 1 else shifted(part, 0, s)
            remote(kv.at[rows], kv.at[rows], kv_s.at[k], kv_r.at[k], dev_plane(to)).wait_recv()

    def zg_ref(direction, n, lag):
        sign = signs[direction]
        if n < 4:
            hop, cols, rows = 0, pl.ds(n * quarter, quarter), pl.ds(0, crows)
        else:
            hop, cols = (n - 2) // 2, pl.ds(n % 2 * chalf, chalf)
            rows = pl.ds(direction * hrows, hrows) if n >= 8 else pl.ds(0, crows)
        return rows_all.at[core, zat(-sign * (hop + lag)), rows, cols]

    def zg(direction, n, lag):
        ref = zg_ref(direction, n, lag)
        return remote(ref, ref, zg_s.at[direction, n], zg_r.at[direction, n], dev_z(signs[direction]))

    def px_ref(direction, a, side):
        d, c = a // 2 + 1, a % 2
        rows = pl.ds(direction * hrows, hrows) if d == 4 else pl.ds(0, crows)
        return rows_all.at[side, zat(-signs[direction] * d), rows, pl.ds(c * chalf, chalf)]

    def px_copy(direction, a):
        ref = px_ref(direction, a, core)
        return remote(ref, ref, px_s.at[direction * 8 + a], px_r.at[direction * 8 + a], partner)

    def px_wait(direction, a):
        ref = px_ref(direction, a, 1 - core)
        remote(ref, ref, px_s.at[direction * 8 + a], px_r.at[direction * 8 + a], partner).wait_recv()

    def arrive(a):
        for direction in (0, 1):
            for n in (2 * a, 2 * a + 1) if a < 2 else (a + 2,):
                zg(direction, n, 1).wait_recv()
            if a < 6:
                zg(direction, a + 4, 0).start()
            px_copy(direction, a).start()

    def ready(d):
        for direction in (0, 1):
            px_wait(direction, 2 * d - 2)
            px_wait(direction, 2 * d - 1)

    def gate_up(zs):
        both = dot(rows_all[0, zs], wgu[:half, :]) + dot(rows_all[1, zs], wgu[half:, :])
        gate, up = both[:, :width], both[:, width:]
        inner_all[core, zs] = (gate / (1.0 + jnp.exp(-gate)) * up).astype(BF)

    def inner_copy(zs):
        ref = inner_all.at[core, zs]
        return remote(ref, ref, in_s.at[zs], in_r.at[zs], partner)

    def inner_wait(zs):
        ref = inner_all.at[1 - core, zs]
        remote(ref, ref, in_s.at[zs], in_r.at[zs], partner).wait_recv()

    def down(zs):
        for c in range(0, half, 512):
            cols = slice(c, c + 512)
            parts[zs, :, cols] = (
                dot(inner_all[0, zs], wd[:width, cols]) + dot(inner_all[1, zs], wd[width:, cols])
            ).astype(BF)

    def pair(f, d):
        @pl.loop(0, 2)
        def _(i):
            f(zat((2 * i - 1) * d))

    col = iota((crows, EXPERTS * SLOT), 1)
    dense = ((col // SLOT) * CAP + lax.rem(col, SLOT) == iota((crows, EXPERTS * SLOT), 0)) & (lax.rem(col, SLOT) < CAP)
    dense = dense.astype(BF)
    kvz_wait(0)
    kvz_go(1)
    keep.wait()
    for c in range(4):
        cols = pl.ds(c * quarter, quarter)
        for i in range(1, EXPERTS):
            ref = a2a_in.at[(*slot_rows(plane_at(EXPERTS - i)), cols)]
            remote(ref, ref, a2a_s.at[c, i], a2a_r.at[c, i], dev_plane(plane_at(i))).wait_recv()
        rows_all[core, z, :, c * quarter : (c + 1) * quarter] = dot(
            dense, a2a_in[:, :, c * quarter : (c + 1) * quarter].astype(F32).reshape(EXPERTS * SLOT, quarter).astype(BF)
        ).astype(BF)
        if c in (0, 1):
            kvz_wait(c + 1)
            kvz_go(c + 2)
        for direction in (0, 1):
            zg(direction, c, 0).start()
    own_ref = rows_all.at[core, z]
    own_px = remote(own_ref, own_ref, px_s.at[16], px_r.at[16], partner)
    own_px.start()
    kvz_wait(3)
    kv_start("s1", "s2own")
    local[3].wait()
    for g in range(groups):
        for h in range(heads):
            i = g * heads + h
            qs[g, h * tok : (h + 1) * tok, :] = qin[:, i * HEAD : (i + 1) * HEAD]
    other_ref = rows_all.at[1 - core, z]
    local[4].wait()
    local[5].wait()
    local[6].wait()

    arrive(0)
    remote(other_ref, other_ref, px_s.at[16], px_r.at[16], partner).wait_recv()
    gate_up(z)
    kv_wait("s1")
    kv_start("f1", "s2a")
    inner_copy(z).start()

    arrive(1)
    inner_wait(z)
    down(z)
    kv_wait("s2own")
    kv_start("f2own")

    arrive(2)
    ready(1)
    pair(gate_up, 1)
    kv_wait("f1")
    kv_start("s2b")
    pair(lambda zs: inner_copy(zs).start(), 1)

    arrive(3)
    pair(inner_wait, 1)
    pair(down, 1)
    kv_wait("s2a")
    kv_start("f2a")

    arrive(4)
    ready(2)
    pair(gate_up, 2)
    pair(lambda zs: inner_copy(zs).start(), 2)

    arrive(5)
    pair(inner_wait, 2)
    pair(down, 2)
    ready(3)
    pair(gate_up, 3)
    pair(lambda zs: inner_copy(zs).start(), 3)

    def rs_rows(direction, chain):
        return pl.ds((direction ^ chain) * hrows, hrows)

    def rs_part(direction, chain, t, c):
        return parts.at[zat(signs[direction] * t), rs_rows(direction, chain), pl.ds(c * chalf, chalf)]

    def rs_slot(direction, chain, t, c):
        return rs_in.at[direction, chain * 4 + t - 1, :, pl.ds(c * chalf, chalf)]

    def rs(direction, chain, t, c):
        n = (chain * 4 + t - 1) * 2 + c
        return remote(
            rs_part(direction, chain, t, c), rs_slot(direction, chain, t, c),
            rs_s.at[direction, n], rs_r.at[direction, n], dev_z(signs[direction]),
        )

    def rs_add(chain, t, c):
        for direction in (0, 1):
            rs(direction, chain, t + 1, c).wait_recv()
            ref = rs_part(direction, chain, t, c)
            ref[...] = (ref[...].astype(F32) + rs_slot(direction, chain, t + 1, c)[...].astype(F32)).astype(BF)

    def rs_go(chain, t, c):
        for direction in (0, 1):
            rs(direction, chain, t, c).start()

    def rs_step(chain, t, c):
        rs_add(chain, t, c)
        rs_go(chain, t, c)

    scale = HEAD ** (-0.5) * LOG2E

    def attend(b, masked):
        rows = pl.ds(pl.multiple_of(b * block_rows, block_rows), block_rows)
        for g in range(groups):
            k = kv[rows, g * HEAD : (g + 1) * HEAD]
            v = kv[rows, kvw + g * HEAD : kvw + (g + 1) * HEAD]
            s = lax.dot_general(qs[g], k, (((1,), (1,)), ((), ())), preferred_element_type=F32) * scale
            if masked:
                row = z * tok + lax.rem(iota(s.shape, 0), tok)
                s = jnp.where(iota(s.shape, 1) <= row, s, NEG)
            tiles = [s[:, j : j + HEAD] for j in range(0, block_rows, HEAD)]
            top = functools.reduce(jnp.maximum, tiles)
            m_old = m_ref[g]
            m_new = jnp.maximum(m_old, jnp.max(top, axis=1, keepdims=True))
            w = [jnp.exp2(t - m_new) for t in tiles]
            f = jnp.exp2(m_old - m_new)
            m_ref[g] = m_new
            l_ref[g] = l_ref[g] * f + functools.reduce(jnp.add, w)
            wb = jnp.concatenate([t.astype(BF) for t in w], axis=1)
            acc_ref[g] = acc_ref[g] * f + dot(wb, v)

    def attend_share(n, of):
        @pl.loop(p * n // of, p * (n + 1) // of)
        def _(b):
            attend(b, False)

    arrive(6)
    pair(inner_wait, 3)
    pair(down, 3)
    rs_go(1, 3, 0)
    rs_go(1, 3, 1)
    arrive(7)
    far = zat(4)
    ready(4)
    gate_up(far)
    inner_copy(far).start()
    kv_wait("s2b")
    kv_start("f2b")
    inner_wait(far)
    down(far)
    kv_wait("f2own")
    rs_go(0, 4, 0)
    rs_step(1, 2, 0)
    rs_go(0, 4, 1)
    rs_step(1, 2, 1)
    attend(p, True)
    kv_wait("f2a")
    rs_step(0, 3, 0)
    kv_wait("f2b")
    attend_share(0, 4)
    rs_step(0, 3, 1)
    rs_step(1, 1, 0)
    attend_share(1, 4)
    rs_step(0, 2, 0)
    rs_step(0, 2, 1)
    attend_share(2, 4)
    rs_step(0, 1, 0)
    rs_step(1, 1, 1)
    rs_step(0, 1, 1)
    attend_share(3, 4)

    srow = iota((EXPERTS * SLOT // 2, hrows), 0)
    spread = ((srow // SLOT) * CAP + lax.rem(srow, SLOT) == iota((EXPERTS * SLOT // 2, hrows), 1)) & (
        lax.rem(srow, SLOT) < CAP
    )
    spread = spread.astype(BF)

    def back(i, c):
        q = plane_at(i)
        cols = pl.ds(c * chalf, chalf)
        return remote(
            back_out.at[(*slot_rows(q), cols)], back_in.at[(*slot_rows(p), cols)], bk_s.at[c, i], bk_r.at[c, i], dev_plane(q)
        )

    def finish(c):
        for direction in (0, 1):
            rs(direction, 1, 1, c).wait_recv()
            rs(direction, 0, 1, c).wait_recv()
        cols = slice(c * chalf, (c + 1) * chalf)
        for h in (0, 1):
            total = parts[z, h * hrows : (h + 1) * hrows, cols].astype(F32)
            for direction in (0, 1):
                total = total + rs_slot(direction, direction ^ h, 1, c)[...].astype(F32)
            n = EXPERTS * SLOT // 2
            back_out[h * (EXPERTS // 2) : (h + 1) * (EXPERTS // 2), :, cols] = (
                dot(spread, total.astype(BF)).reshape(EXPERTS // 2, SLOT, chalf).astype(BF)
            )
        stay = pltpu.make_async_copy(
            back_out.at[(*slot_rows(p), pl.ds(c * chalf, chalf))],
            back_in.at[(*slot_rows(p), pl.ds(c * chalf, chalf))],
            local_sem.at[8 + c],
        )
        stay.start()
        for i in range(1, EXPERTS):
            back(i, c).start()
        return stay

    def mix(c, stay):
        for i in range(1, EXPERTS):
            ref = back_in.at[(*slot_rows(plane_at(EXPERTS - i)), pl.ds(c * chalf, chalf))]
            remote(ref, ref, bk_s.at[c, i], bk_r.at[c, i], dev_plane(plane_at(i))).wait_recv()
        stay.wait()
        for b in range(c * chalf, (c + 1) * chalf, quarter):
            own = dot(
                sel_ref[...], back_in[:, :, b : b + quarter].astype(F32).reshape(EXPERTS * SLOT, quarter).astype(BF)
            )
            for t in range(0, quarter, HEAD):
                mix_ref[:, b + t : b + t + HEAD] = (own[:, t : t + HEAD] * gain_col[...]).astype(BF)

    first = finish(0)
    for g in range(groups):
        out = acc_ref[g] / jnp.sum(l_ref[g], axis=1, keepdims=True)
        for h in range(heads):
            i = g * heads + h
            att_ref[:, i * HEAD : (i + 1) * HEAD] = out[h * tok : (h + 1) * tok].astype(BF)
    second = finish(1)
    att_out = pltpu.make_async_copy(att_ref, att_hbm, local_sem.at[10])
    att_out.start()

    for c in range(4):
        for i in range(1, EXPERTS):
            a2a(i, c).wait_send()
    for direction in (0, 1):
        for n in range(4):
            kvz(direction, n, 0).wait_send()
        for n in range(10):
            zg(direction, n, 0).wait_send()
        for a in range(8):
            px_copy(direction, a).wait_send()
        for c in (0, 1):
            for t in (4, 3, 2, 1):
                rs(direction, 0, t, c).wait_send()
            for t in (3, 2, 1):
                rs(direction, 1, t, c).wait_send()
    own_px.wait_send()
    for zs in range(HOSTS):
        inner_copy(zs).wait_send()
    for name in stages:
        for c in stages[name]:
            kv_copy(*c).wait_send()

    mix(0, first)
    mix_out = [
        pltpu.make_async_copy(
            mix_ref.at[:, pl.ds(c * chalf, chalf)], mix_hbm.at[:, pl.ds(c * chalf, chalf)], local_sem.at[11 + c]
        )
        for c in (0, 1)
    ]
    mix_out[0].start()
    mix(1, second)
    mix_out[1].start()
    att_out.wait()
    mix_out[0].wait()
    mix_out[1].wait()
    for c in (0, 1):
        for i in range(1, EXPERTS):
            back(i, c).wait_send()


def closing(a_ref, b_ref, a_out, b_out):
    a_out[...] = a_ref[...]
    b_out[...] = b_ref[...]


def body(queries, keys, values, hidden, route_ids, route_gain, w_gate, w_up, w_down):
    tok, half = hidden.shape
    width_q, kvw = queries.shape[1], keys.shape[1]
    ff = w_gate.shape[2]
    total = tok * HOSTS * EXPERTS
    crows = EXPERTS * CAP
    groups = kvw // HEAD
    qrows = width_q // kvw * tok
    vm = pl.BlockSpec(memory_space=pltpu.VMEM)
    hbm = pl.BlockSpec(memory_space=pl.ANY)
    dma = pltpu.SemaphoreType.DMA
    attended, mixed = pl.pallas_call(
        kernel,
        name="layer",
        out_shape=(
            jax.ShapeDtypeStruct((tok, width_q), BF),
            jax.ShapeDtypeStruct((tok, half), BF),
        ),
        in_specs=[vm, vm] + [hbm] * 7,
        out_specs=(hbm, hbm),
        scratch_shapes=[
            pltpu.VMEM((tok, width_q), BF),
            pltpu.VMEM((tok, half), BF),
            pltpu.VMEM((tok, half), BF),
            pltpu.VMEM((tok, width_q), BF),
            pltpu.VMEM((EXPERTS, SLOT, half), BF),
            pltpu.VMEM((EXPERTS, SLOT, half), BF),
            pltpu.VMEM((2, HOSTS, crows, half), BF),
            pltpu.VMEM((2 * half, 2 * ff), BF),
            pltpu.VMEM((2 * ff, half), BF),
            pltpu.VMEM((2, HOSTS, crows, ff), BF),
            pltpu.VMEM((HOSTS, crows, half), BF),
            pltpu.VMEM((2, 7, crows // 2, half), BF),
            pltpu.VMEM((EXPERTS, SLOT, half), BF),
            pltpu.VMEM((EXPERTS, SLOT, half), BF),
            pltpu.VMEM((tok, EXPERTS * SLOT), BF),
            pltpu.VMEM((tok, HEAD), F32),
            pltpu.VMEM((total, 2 * kvw), BF),
            pltpu.VMEM((groups, qrows, HEAD), BF),
            pltpu.VMEM((groups, qrows, HEAD), F32),
            pltpu.VMEM((groups, qrows, HEAD), F32),
            pltpu.VMEM((groups, qrows, HEAD), F32),
            dma((13,)),
            dma((4, EXPERTS)), dma((4, EXPERTS)),
            dma((2, 4)), dma((2, 4)),
            dma((2, 10)), dma((2, 10)),
            dma((17,)), dma((17,)),
            dma((HOSTS,)), dma((HOSTS,)),
            dma((44,)), dma((44,)),
            dma((2, 14)), dma((2, 14)),
            dma((2, EXPERTS)), dma((2, EXPERTS)),
        ],
        compiler_params=pltpu.CompilerParams(
            collective_id=0, has_side_effects=True, vmem_limit_bytes=60 * 1024 * 1024
        ),
    )(route_ids.reshape(1, tok), route_gain.reshape(1, tok), hidden, queries, keys, values, w_gate, w_up, w_down)
    return pl.pallas_call(
        closing,
        name="closing",
        out_shape=(jax.ShapeDtypeStruct((tok, width_q), BF), jax.ShapeDtypeStruct((tok, half), BF)),
        in_specs=[vm, vm],
        out_specs=(vm, vm),
    )(attended, mixed)


def solution(mesh):
    in_specs = (
        P("ctx", "tp"),
        P("ctx", "tp"),
        P("ctx", "tp"),
        P("ctx", "tp"),
        P("ctx", None),
        P("ctx"),
        P("ctx", None, "tp"),
        P("ctx", None, "tp"),
        P("ctx", None, "tp"),
    )
    out_specs = (P("ctx", "tp"), P("ctx", "tp"))
    return jax.shard_map(body, mesh=mesh, in_specs=in_specs, out_specs=out_specs, check_vma=False)
```

```python
import functools

import jax
import jax.numpy as jnp
from jax import lax
from jax.experimental import pallas as pl
from jax.experimental.pallas import tpu as pltpu
from jax.sharding import PartitionSpec as P

HEAD = 128
EXPERTS = 16
SIDE = 4
HOSTS = 8
CAP = 6
SLOT = 8
LOG2E = 1.4426950408889634
NEG = -1e30
MESH = pl.DeviceIdType.MESH
BF = jnp.bfloat16
F32 = jnp.float32


def iota(shape, dim):
    return lax.broadcasted_iota(jnp.int32, shape, dim)


def dot(a, b):
    return jnp.dot(a, b, preferred_element_type=F32)


def kernel(
    ids_ref, gain_ref, hidden_ref, q_ref, keys_ref, values_ref, wg_ref, wu_ref, wd_ref,
    att_hbm, mix_hbm,
    att_ref, mix_ref, hid, qin, packed, a2a_in, rows_all, wgu, wd, inner_all, parts, rs_in, back_out, back_in, sel_ref, gain_col,
    kv, qs, m_ref, l_ref, acc_ref,
    local_sem, a2a_s, a2a_r, kvz_s, kvz_r, zg_s, zg_r, px_s, px_r, in_s, in_r, kv_s, kv_r, rs_s, rs_r, bk_s, bk_r,
):
    tok, half = hidden_ref.shape
    me = lax.axis_index("ctx")
    core = lax.axis_index("tp")
    z = lax.rem(me, HOSTS)
    p = me // HOSTS
    px, py = p // SIDE, lax.rem(p, SIDE)
    crows = EXPERTS * CAP
    hrows = crows // 2
    block_rows = HOSTS * tok
    kvw = keys_ref.shape[1]
    groups = kvw // HEAD
    heads = q_ref.shape[1] // HEAD // groups
    width = wg_ref.shape[2]
    chalf, quarter = half // 2, half // 4
    group = ((0, 1536), (1536, half - 1536))

    def zat(d):
        return lax.rem(z + d + HOSTS, HOSTS)

    def dev_z(d):
        return {"ctx": p * HOSTS + zat(d), "tp": core}

    def plane_at(i):
        return lax.rem(px + i // SIDE, SIDE) * SIDE + lax.rem(py + i % SIDE, SIDE)

    def plane_from(i):
        return lax.rem(px + SIDE - i // SIDE, SIDE) * SIDE + lax.rem(py + SIDE - i % SIDE, SIDE)

    def hops(i):
        return min(i // SIDE, SIDE - i // SIDE) + min(i % SIDE, SIDE - i % SIDE)

    shifts = sorted(range(1, EXPERTS), key=lambda i: -hops(i))

    def dev_plane(q):
        return {"ctx": q * HOSTS + z, "tp": core}

    partner = {"ctx": me, "tp": 1 - core}
    signs = (1, -1)

    def remote(src, dst, s, r, device):
        return pltpu.make_async_remote_copy(
            src_ref=src, dst_ref=dst, send_sem=s, recv_sem=r, device_id=device, device_id_type=MESH
        )

    barrier = pltpu.get_barrier_semaphore()
    greeted = [dev_plane(plane_at(i)) for i in shifts] + [dev_z(1), dev_z(-1), partner]
    for device in greeted:
        pl.semaphore_signal(barrier, inc=1, device_id=device, device_id_type=MESH)

    own_rows = pl.ds(pl.multiple_of(me * tok, tok), tok)
    local = [
        pltpu.make_async_copy(hidden_ref, hid, local_sem.at[0]),
        pltpu.make_async_copy(keys_ref, kv.at[own_rows, pl.ds(0, kvw)], local_sem.at[1]),
        pltpu.make_async_copy(values_ref, kv.at[own_rows, pl.ds(kvw, kvw)], local_sem.at[2]),
        pltpu.make_async_copy(q_ref, qin, local_sem.at[3]),
        pltpu.make_async_copy(wg_ref.at[0], wgu.at[:, pl.ds(0, width)], local_sem.at[4]),
        pltpu.make_async_copy(wu_ref.at[0], wgu.at[:, pl.ds(width, width)], local_sem.at[5]),
        pltpu.make_async_copy(wd_ref.at[0], wd, local_sem.at[6]),
    ]
    for c in local:
        c.start()

    ids = ids_ref[...]
    chosen = (ids == iota((EXPERTS, tok), 0)).astype(F32)
    before = (iota((tok, tok), 0) < iota((tok, tok), 1)).astype(BF)
    rank = jnp.sum(dot(chosen.astype(BF), before) * chosen, axis=0, keepdims=True).astype(jnp.int32)
    sel = (ids * SLOT + rank == iota((EXPERTS * SLOT, tok), 0)).astype(F32)
    sel_ref[...] = sel.T.astype(BF)
    gain_col[...] = jnp.broadcast_to(gain_ref[...], (HEAD, tok)).T
    sel = sel.astype(BF)
    local[0].wait()
    for c in range(0, half, quarter):
        packed[:, :, c : c + quarter] = dot(sel, hid[:, c : c + quarter]).reshape(EXPERTS, SLOT, quarter).astype(BF)
    m_ref[...] = jnp.full_like(m_ref, NEG)
    l_ref[...] = jnp.zeros_like(l_ref)
    acc_ref[...] = jnp.zeros_like(acc_ref)
    unread = jnp.zeros((EXPERTS, SLOT - CAP, half), BF)
    a2a_in[:, CAP:, :] = unread
    back_in[:, CAP:, :] = unread
    local[1].wait()
    local[2].wait()

    pl.semaphore_wait(barrier, len(greeted))

    def kvz(direction, n, lag):
        sign = signs[direction]
        start = (p * HOSTS + zat(-sign * (n + lag))) * tok
        if n == 3:
            rows = pl.ds(pl.multiple_of(start + direction * (tok // 2), tok // 2), tok // 2)
        else:
            rows = pl.ds(pl.multiple_of(start, tok), tok)
        return remote(kv.at[rows], kv.at[rows], kvz_s.at[direction, n], kvz_r.at[direction, n], dev_z(sign))

    def kvz_go(n):
        for direction in (0, 1):
            kvz(direction, n, 0).start()

    def kvz_wait(n):
        for direction in (0, 1):
            kvz(direction, n, 1).wait_recv()

    kvz_go(0)

    def slot_rows(q):
        return q, pl.ds(0, CAP)

    def a2a(i, c):
        q = plane_at(i)
        cols = pl.ds(c * quarter, quarter)
        return remote(
            packed.at[(*slot_rows(q), cols)], a2a_in.at[(*slot_rows(p), cols)], a2a_s.at[c, i], a2a_r.at[c, i], dev_plane(q)
        )

    keep = pltpu.make_async_copy(packed.at[slot_rows(p)], a2a_in.at[slot_rows(p)], local_sem.at[7])
    keep.start()
    for c in range(4):
        for i in shifts:
            a2a(i, c).start()

    def shifted(part, d1, d2):
        dx, dy = (d1, d2) if part == 0 else (d2, d1)
        return lax.rem(px + dx + SIDE, SIDE) * SIDE + lax.rem(py + dy + SIDE, SIDE)

    part_rows = block_rows // 2
    unit = part_rows // 2
    kv_copies = {}

    def kv_copy(name, part, along, s, d1, d2, off, n):
        if name not in kv_copies:
            kv_copies[name] = len(kv_copies)
        k = kv_copies[name]
        rows = pl.ds(pl.multiple_of(shifted(part, d1, d2) * block_rows + part * part_rows + off, unit), n)
        to = shifted(part, s, 0) if along == 1 else shifted(part, 0, s)
        return remote(kv.at[rows], kv.at[rows], kv_s.at[k], kv_r.at[k], dev_plane(to))

    stages = {}
    for part in (0, 1):
        for s in (1, -1):
            fo = 0 if s == 1 else unit
            stages.setdefault("s1", []).append((("s1", part, s), part, 1, s, 0, 0, 0, part_rows))
            stages.setdefault("s2own", []).append((("s2own", part, s), part, 2, s, 0, 0, 0, part_rows))
            stages.setdefault("f1", []).append((("f1", part, s), part, 1, s, -s, 0, fo, unit))
            for d1 in (-1, 1):
                stages.setdefault("s2a", []).append((("s2a", part, s, d1), part, 2, s, d1, 0, 0, part_rows))
            stages.setdefault("f2own", []).append((("f2own", part, s), part, 2, s, 0, -s, fo, unit))
            for off in (0, unit):
                stages.setdefault("s2b", []).append((("s2b", part, s, off), part, 2, s, 2, 0, off, unit))
            for d1 in (-1, 1):
                stages.setdefault("f2a", []).append((("f2a", part, s, d1), part, 2, s, d1, -s, fo, unit))
            stages.setdefault("f2b", []).append((("f2b", part, s), part, 2, s, 2, -s, fo, unit))

    def kv_start(*names):
        for name in names:
            for c in stages[name]:
                kv_copy(*c).start()

    def kv_wait(name):
        for key, part, along, s, d1, d2, off, n in stages[name]:
            e1, e2 = (d1 - s, d2) if along == 1 else (d1, d2 - s)
            k = kv_copies[key]
            rows = pl.ds(pl.multiple_of(shifted(part, e1, e2) * block_rows + part * part_rows + off, unit), n)
            to = shifted(part, s, 0) if along == 1 else shifted(part, 0, s)
            remote(kv.at[rows], kv.at[rows], kv_s.at[k], kv_r.at[k], dev_plane(to)).wait_recv()

    def zg_ref(direction, n, lag):
        sign = signs[direction]
        if n < 4:
            hop, cols, rows = 0, pl.ds(n * quarter, quarter), pl.ds(0, crows)
        else:
            hop, cols = (n - 2) // 2, pl.ds(n % 2 * chalf, chalf)
            rows = pl.ds(direction * hrows, hrows) if n >= 8 else pl.ds(0, crows)
        return rows_all.at[core, zat(-sign * (hop + lag)), rows, cols]

    def zg(direction, n, lag):
        ref = zg_ref(direction, n, lag)
        return remote(ref, ref, zg_s.at[direction, n], zg_r.at[direction, n], dev_z(signs[direction]))

    def px_ref(direction, a, side):
        d, c = a // 2 + 1, a % 2
        rows = pl.ds(direction * hrows, hrows) if d == 4 else pl.ds(0, crows)
        return rows_all.at[side, zat(-signs[direction] * d), rows, pl.ds(c * chalf, chalf)]

    def px_copy(direction, a):
        ref = px_ref(direction, a, core)
        return remote(ref, ref, px_s.at[direction * 8 + a], px_r.at[direction * 8 + a], partner)

    def px_wait(direction, a):
        ref = px_ref(direction, a, 1 - core)
        remote(ref, ref, px_s.at[direction * 8 + a], px_r.at[direction * 8 + a], partner).wait_recv()

    def arrive(a):
        for direction in (0, 1):
            for n in (2 * a, 2 * a + 1) if a < 2 else (a + 2,):
                zg(direction, n, 1).wait_recv()
            if a < 6:
                zg(direction, a + 4, 0).start()
            px_copy(direction, a).start()

    def ready(d):
        for direction in (0, 1):
            px_wait(direction, 2 * d - 2)
            px_wait(direction, 2 * d - 1)

    def gate_up(zs):
        both = dot(rows_all[0, zs], wgu[:half, :]) + dot(rows_all[1, zs], wgu[half:, :])
        gate, up = both[:, :width], both[:, width:]
        inner_all[core, zs] = (gate / (1.0 + jnp.exp(-gate)) * up).astype(BF)

    def inner_copy(zs):
        ref = inner_all.at[core, zs]
        return remote(ref, ref, in_s.at[zs], in_r.at[zs], partner)

    def inner_wait(zs):
        ref = inner_all.at[1 - core, zs]
        remote(ref, ref, in_s.at[zs], in_r.at[zs], partner).wait_recv()

    def down(zs):
        for c in range(0, half, 512):
            cols = slice(c, c + 512)
            parts[zs, :, cols] = (
                dot(inner_all[0, zs], wd[:width, cols]) + dot(inner_all[1, zs], wd[width:, cols])
            ).astype(BF)

    def pair(f, d):
        @pl.loop(0, 2)
        def _(i):
            f(zat((2 * i - 1) * d))

    col = iota((crows, EXPERTS * SLOT), 1)
    dense = ((col // SLOT) * CAP + lax.rem(col, SLOT) == iota((crows, EXPERTS * SLOT), 0)) & (lax.rem(col, SLOT) < CAP)
    dense = dense.astype(BF)
    kvz_wait(0)
    kvz_go(1)
    keep.wait()
    for c in range(4):
        cols = pl.ds(c * quarter, quarter)
        for i in shifts:
            ref = a2a_in.at[(*slot_rows(plane_from(i)), cols)]
            remote(ref, ref, a2a_s.at[c, i], a2a_r.at[c, i], dev_plane(plane_at(i))).wait_recv()
        rows_all[core, z, :, c * quarter : (c + 1) * quarter] = dot(
            dense, a2a_in[:, :, c * quarter : (c + 1) * quarter].astype(F32).reshape(EXPERTS * SLOT, quarter).astype(BF)
        ).astype(BF)
        if c in (0, 1):
            kvz_wait(c + 1)
            kvz_go(c + 2)
        for direction in (0, 1):
            zg(direction, c, 0).start()
    own_ref = rows_all.at[core, z]
    own_px = remote(own_ref, own_ref, px_s.at[16], px_r.at[16], partner)
    own_px.start()
    kvz_wait(3)
    kv_start("s1", "s2own")
    local[3].wait()
    for g in range(groups):
        for h in range(heads):
            i = g * heads + h
            qs[g, h * tok : (h + 1) * tok, :] = qin[:, i * HEAD : (i + 1) * HEAD]
    other_ref = rows_all.at[1 - core, z]
    local[4].wait()
    local[5].wait()
    local[6].wait()

    arrive(0)
    remote(other_ref, other_ref, px_s.at[16], px_r.at[16], partner).wait_recv()
    gate_up(z)
    kv_wait("s1")
    kv_start("f1", "s2a")
    inner_copy(z).start()

    arrive(1)
    inner_wait(z)
    down(z)
    kv_wait("s2own")
    kv_start("f2own")

    arrive(2)
    ready(1)
    pair(gate_up, 1)
    kv_wait("f1")
    kv_start("s2b")
    pair(lambda zs: inner_copy(zs).start(), 1)

    arrive(3)
    pair(inner_wait, 1)
    pair(down, 1)

    arrive(4)
    ready(2)
    pair(gate_up, 2)
    pair(lambda zs: inner_copy(zs).start(), 2)

    arrive(5)
    pair(inner_wait, 2)
    pair(down, 2)
    kv_wait("s2a")
    kv_start("f2a")
    ready(3)
    pair(gate_up, 3)
    pair(lambda zs: inner_copy(zs).start(), 3)

    def rs_rows(direction, chain):
        return pl.ds((direction ^ chain) * hrows, hrows)

    def rs_part(direction, chain, t, c):
        return parts.at[zat(signs[direction] * t), rs_rows(direction, chain), pl.ds(*group[c])]

    def rs_slot(direction, chain, t, c):
        return rs_in.at[direction, chain * 4 + t - 1, :, pl.ds(*group[c])]

    def rs(direction, chain, t, c):
        n = (chain * 4 + t - 1) * 2 + c
        return remote(
            rs_part(direction, chain, t, c), rs_slot(direction, chain, t, c),
            rs_s.at[direction, n], rs_r.at[direction, n], dev_z(signs[direction]),
        )

    def rs_add(chain, t, c):
        for direction in (0, 1):
            rs(direction, chain, t + 1, c).wait_recv()
            ref = rs_part(direction, chain, t, c)
            ref[...] = (ref[...].astype(F32) + rs_slot(direction, chain, t + 1, c)[...].astype(F32)).astype(BF)

    def rs_go(chain, t, c):
        for direction in (0, 1):
            rs(direction, chain, t, c).start()

    def rs_step(chain, t, c):
        rs_add(chain, t, c)
        rs_go(chain, t, c)

    scale = HEAD ** (-0.5) * LOG2E

    def attend(b, masked):
        rows = pl.ds(pl.multiple_of(b * block_rows, block_rows), block_rows)
        for g in range(groups):
            k = kv[rows, g * HEAD : (g + 1) * HEAD]
            v = kv[rows, kvw + g * HEAD : kvw + (g + 1) * HEAD]
            s = lax.dot_general(qs[g], k, (((1,), (1,)), ((), ())), preferred_element_type=F32) * scale
            if masked:
                row = z * tok + lax.rem(iota(s.shape, 0), tok)
                s = jnp.where(iota(s.shape, 1) <= row, s, NEG)
            tiles = [s[:, j : j + HEAD] for j in range(0, block_rows, HEAD)]
            top = functools.reduce(jnp.maximum, tiles)
            m_old = m_ref[g]
            m_new = jnp.maximum(m_old, jnp.max(top, axis=1, keepdims=True))
            w = [jnp.exp2(t - m_new) for t in tiles]
            f = jnp.exp2(m_old - m_new)
            m_ref[g] = m_new
            l_ref[g] = l_ref[g] * f + functools.reduce(jnp.add, w)
            wb = jnp.concatenate([t.astype(BF) for t in w], axis=1)
            acc_ref[g] = acc_ref[g] * f + dot(wb, v)

    def attend_share(n, of):
        @pl.loop(p * n // of, p * (n + 1) // of)
        def _(b):
            attend(b, False)

    arrive(6)
    pair(inner_wait, 3)
    pair(down, 3)
    rs_go(1, 3, 0)
    rs_go(1, 3, 1)
    arrive(7)
    far = zat(4)
    ready(4)
    gate_up(far)
    inner_copy(far).start()
    kv_wait("s2b")
    kv_start("f2b")
    inner_wait(far)
    down(far)
    kv_wait("f2own")
    rs_go(0, 4, 0)
    rs_step(1, 2, 0)
    rs_go(0, 4, 1)
    rs_step(1, 2, 1)
    attend(p, True)
    kv_wait("f2a")
    rs_step(0, 3, 0)
    kv_wait("f2b")
    attend_share(0, 4)
    rs_step(0, 3, 1)
    rs_step(1, 1, 0)
    attend_share(1, 4)
    rs_step(0, 2, 0)
    rs_step(0, 2, 1)
    attend_share(2, 4)
    rs_step(0, 1, 0)
    rs_step(1, 1, 1)
    rs_step(0, 1, 1)
    attend_share(3, 4)

    srow = iota((EXPERTS * SLOT // 2, hrows), 0)
    spread = ((srow // SLOT) * CAP + lax.rem(srow, SLOT) == iota((EXPERTS * SLOT // 2, hrows), 1)) & (
        lax.rem(srow, SLOT) < CAP
    )
    spread = spread.astype(BF)

    def back(i, c):
        q = plane_at(i)
        cols = pl.ds(*group[c])
        return remote(
            back_out.at[(*slot_rows(q), cols)], back_in.at[(*slot_rows(p), cols)], bk_s.at[c, i], bk_r.at[c, i], dev_plane(q)
        )

    def finish(c):
        for direction in (0, 1):
            rs(direction, 1, 1, c).wait_recv()
            rs(direction, 0, 1, c).wait_recv()
        cols = slice(group[c][0], sum(group[c]))
        for h in (0, 1):
            total = parts[z, h * hrows : (h + 1) * hrows, cols].astype(F32)
            for direction in (0, 1):
                total = total + rs_slot(direction, direction ^ h, 1, c)[...].astype(F32)
            n = EXPERTS * SLOT // 2
            back_out[h * (EXPERTS // 2) : (h + 1) * (EXPERTS // 2), :, cols] = (
                dot(spread, total.astype(BF)).reshape(EXPERTS // 2, SLOT, group[c][1]).astype(BF)
            )
        stay = pltpu.make_async_copy(
            back_out.at[(*slot_rows(p), pl.ds(*group[c]))],
            back_in.at[(*slot_rows(p), pl.ds(*group[c]))],
            local_sem.at[8 + c],
        )
        stay.start()
        for i in shifts:
            back(i, c).start()
        return stay

    def mix(c, stay):
        for i in shifts:
            ref = back_in.at[(*slot_rows(plane_from(i)), pl.ds(*group[c]))]
            remote(ref, ref, bk_s.at[c, i], bk_r.at[c, i], dev_plane(plane_at(i))).wait_recv()
        stay.wait()
        for b in range(group[c][0], sum(group[c]), 512):
            own = dot(
                sel_ref[...], back_in[:, :, b : b + 512].astype(F32).reshape(EXPERTS * SLOT, 512).astype(BF)
            )
            for t in range(0, 512, HEAD):
                mix_ref[:, b + t : b + t + HEAD] = (own[:, t : t + HEAD] * gain_col[...]).astype(BF)

    first = finish(0)
    for g in range(groups):
        out = acc_ref[g] / jnp.sum(l_ref[g], axis=1, keepdims=True)
        for h in range(heads):
            i = g * heads + h
            att_ref[:, i * HEAD : (i + 1) * HEAD] = out[h * tok : (h + 1) * tok].astype(BF)
    second = finish(1)
    att_out = pltpu.make_async_copy(att_ref, att_hbm, local_sem.at[10])
    att_out.start()

    for c in range(4):
        for i in shifts:
            a2a(i, c).wait_send()
    for direction in (0, 1):
        for n in range(4):
            kvz(direction, n, 0).wait_send()
        for n in range(10):
            zg(direction, n, 0).wait_send()
        for a in range(8):
            px_copy(direction, a).wait_send()
        for c in (0, 1):
            for t in (4, 3, 2, 1):
                rs(direction, 0, t, c).wait_send()
            for t in (3, 2, 1):
                rs(direction, 1, t, c).wait_send()
    own_px.wait_send()
    for zs in range(HOSTS):
        inner_copy(zs).wait_send()
    for name in stages:
        for c in stages[name]:
            kv_copy(*c).wait_send()

    mix(0, first)
    mix_out = [
        pltpu.make_async_copy(
            mix_ref.at[:, pl.ds(*group[c])], mix_hbm.at[:, pl.ds(*group[c])], local_sem.at[11 + c]
        )
        for c in (0, 1)
    ]
    mix_out[0].start()
    mix(1, second)
    mix_out[1].start()
    att_out.wait()
    mix_out[0].wait()
    mix_out[1].wait()
    for c in (0, 1):
        for i in shifts:
            back(i, c).wait_send()


def closing(a_ref, b_ref, a_out, b_out):
    a_out[...] = a_ref[...]
    b_out[...] = b_ref[...]


def body(queries, keys, values, hidden, route_ids, route_gain, w_gate, w_up, w_down):
    tok, half = hidden.shape
    width_q, kvw = queries.shape[1], keys.shape[1]
    ff = w_gate.shape[2]
    total = tok * HOSTS * EXPERTS
    crows = EXPERTS * CAP
    groups = kvw // HEAD
    qrows = width_q // kvw * tok
    vm = pl.BlockSpec(memory_space=pltpu.VMEM)
    hbm = pl.BlockSpec(memory_space=pl.ANY)
    dma = pltpu.SemaphoreType.DMA
    attended, mixed = pl.pallas_call(
        kernel,
        name="layer",
        out_shape=(
            jax.ShapeDtypeStruct((tok, width_q), BF),
            jax.ShapeDtypeStruct((tok, half), BF),
        ),
        in_specs=[vm, vm] + [hbm] * 7,
        out_specs=(hbm, hbm),
        scratch_shapes=[
            pltpu.VMEM((tok, width_q), BF),
            pltpu.VMEM((tok, half), BF),
            pltpu.VMEM((tok, half), BF),
            pltpu.VMEM((tok, width_q), BF),
            pltpu.VMEM((EXPERTS, SLOT, half), BF),
            pltpu.VMEM((EXPERTS, SLOT, half), BF),
            pltpu.VMEM((2, HOSTS, crows, half), BF),
            pltpu.VMEM((2 * half, 2 * ff), BF),
            pltpu.VMEM((2 * ff, half), BF),
            pltpu.VMEM((2, HOSTS, crows, ff), BF),
            pltpu.VMEM((HOSTS, crows, half), BF),
            pltpu.VMEM((2, 7, crows // 2, half), BF),
            pltpu.VMEM((EXPERTS, SLOT, half), BF),
            pltpu.VMEM((EXPERTS, SLOT, half), BF),
            pltpu.VMEM((tok, EXPERTS * SLOT), BF),
            pltpu.VMEM((tok, HEAD), F32),
            pltpu.VMEM((total, 2 * kvw), BF),
            pltpu.VMEM((groups, qrows, HEAD), BF),
            pltpu.VMEM((groups, qrows, HEAD), F32),
            pltpu.VMEM((groups, qrows, HEAD), F32),
            pltpu.VMEM((groups, qrows, HEAD), F32),
            dma((13,)),
            dma((4, EXPERTS)), dma((4, EXPERTS)),
            dma((2, 4)), dma((2, 4)),
            dma((2, 10)), dma((2, 10)),
            dma((17,)), dma((17,)),
            dma((HOSTS,)), dma((HOSTS,)),
            dma((44,)), dma((44,)),
            dma((2, 14)), dma((2, 14)),
            dma((2, EXPERTS)), dma((2, EXPERTS)),
        ],
        compiler_params=pltpu.CompilerParams(
            collective_id=0, has_side_effects=True, vmem_limit_bytes=60 * 1024 * 1024
        ),
    )(route_ids.reshape(1, tok), route_gain.reshape(1, tok), hidden, queries, keys, values, w_gate, w_up, w_down)
    return pl.pallas_call(
        closing,
        name="closing",
        out_shape=(jax.ShapeDtypeStruct((tok, width_q), BF), jax.ShapeDtypeStruct((tok, half), BF)),
        in_specs=[vm, vm],
        out_specs=(vm, vm),
    )(attended, mixed)


def solution(mesh):
    in_specs = (
        P("ctx", "tp"),
        P("ctx", "tp"),
        P("ctx", "tp"),
        P("ctx", "tp"),
        P("ctx", None),
        P("ctx"),
        P("ctx", None, "tp"),
        P("ctx", None, "tp"),
        P("ctx", None, "tp"),
    )
    out_specs = (P("ctx", "tp"), P("ctx", "tp"))
    return jax.shard_map(body, mesh=mesh, in_specs=in_specs, out_specs=out_specs, check_vma=False)
```
